32 devices in a mesh: data: 1 (over z), col: 4 (over y), row: 8 (over x, core).
Axes of the slice: x: 4, y: 4, z: 1, core: 2. Of those that a mesh axis runs over, the one named last changes fastest.
The devices are a block of a 4x4x8 slice.
Arguments:
- tokens: bfloat16 [4096, 8192], P(('data', 'row'), 'col')
- w_qkv: bfloat16 [8192, 10240], P('row', 'col')
- w_out: bfloat16 [8192, 8192], P('row', 'col')
- doc_ids: int32 [4096], P(('data', 'row'))
Outputs:
- output: bfloat16 [4096, 8192], P(('data', 'row'), 'col')
All inputs are finite; a program needn't handle non-finite values.
Results may differ from the reference program's by a relative error of at most 0.00445.
Values are sent between devices in bfloat16 or wider.
A program may use at most 768 MiB of HBM per device.

```python
import jax
import jax.numpy as jnp
from jax import lax

HIDDEN = 8192
N_HEADS = 64
KV_HEADS = 8
HEAD_DIM = 128
SEQ_LEN = 4096
N_DOCS = 4

GROUP_RATIO = N_HEADS // KV_HEADS
QKV_COLS = HIDDEN + 2 * KV_HEADS * HEAD_DIM


def block_size(row_count, score_width):
    q_blk = row_count
    while q_blk % 16 == 0 and q_blk * score_width > 4194304:
        q_blk = q_blk // 2
    return q_blk


def setup_inputs(seed: int = 0, part: int = 0) -> dict:
    base_key = jax.random.key(seed)
    key_qkv, key_out, key_part = jax.random.split(base_key, 3)
    part_key = jax.random.fold_in(key_part, part)
    key_tok, key_doc = jax.random.split(part_key)
    tokens = jax.random.normal(key_tok, (SEQ_LEN, HIDDEN), jnp.float32).astype(jnp.bfloat16)
    w_qkv = (jax.random.normal(key_qkv, (HIDDEN, QKV_COLS), jnp.float32) * HIDDEN ** -0.5).astype(jnp.bfloat16)
    w_out = (jax.random.normal(key_out, (HIDDEN, HIDDEN), jnp.float32) * HIDDEN ** -0.5).astype(jnp.bfloat16)
    doc_cuts = jax.random.randint(key_doc, (N_DOCS - 1,), 1, SEQ_LEN, dtype=jnp.int32)
    positions = jnp.arange(SEQ_LEN, dtype=jnp.int32)
    doc_ids = jnp.sum((positions[:, None] >= doc_cuts[None, :]).astype(jnp.int32), axis=1)
    return {"tokens": tokens, "w_qkv": w_qkv, "w_out": w_out, "doc_ids": doc_ids}


def reference(tokens, w_qkv, w_out, doc_ids):
    qkv_rows = jnp.dot(tokens, w_qkv, preferred_element_type=jnp.float32).astype(jnp.bfloat16)
    qkv_rows = qkv_rows.reshape(SEQ_LEN, KV_HEADS, GROUP_RATIO + 2, HEAD_DIM)
    key_rows = qkv_rows[:, :, GROUP_RATIO, :].astype(jnp.float32)
    value_rows = qkv_rows[:, :, GROUP_RATIO + 1, :].astype(jnp.float32)
    q_blk = block_size(SEQ_LEN, N_HEADS * SEQ_LEN)
    n_steps = SEQ_LEN // q_blk
    q_steps = qkv_rows[:, :, :GROUP_RATIO, :].reshape(n_steps, q_blk, KV_HEADS, GROUP_RATIO, HEAD_DIM)
    score_scale = HEAD_DIM ** -0.5

    def attend(block_in):
        q_part, seg_part = block_in
        scores = jnp.einsum("qgrd,kgd->qgrk", q_part.astype(jnp.float32), key_rows) * score_scale
        same_doc = seg_part[:, None, None, None] == doc_ids[None, None, None, :]
        scores = jnp.where(same_doc, scores, -jnp.inf)
        weights = jax.nn.softmax(scores, axis=-1).astype(jnp.bfloat16)
        context = jnp.einsum("qgrk,kgd->qgrd", weights.astype(jnp.float32), value_rows)
        return context.astype(jnp.bfloat16)

    context = lax.map(attend, (q_steps, doc_ids.reshape(n_steps, q_blk)))
    context = context.reshape(SEQ_LEN, HIDDEN)
    return jnp.dot(context, w_out, preferred_element_type=jnp.float32).astype(jnp.bfloat16)
```

```python
import functools

import jax
import jax.numpy as jnp
from jax import lax
from jax.experimental import pallas as pl
from jax.experimental.pallas import tpu as pltpu
from jax.sharding import PartitionSpec as P

HEAD_DIM = 128
CORES = 2
Q_TILE = 256
LOG2E = 1.4426950408889634


def attention_kernel(flag_ref, order_ref, segq_ref, segk_ref, q_ref, k_ref, v_ref, o_ref, m_ref, l_ref, acc_ref):
    tile = pl.program_id(0)
    n_blk, _, k_blk = segk_ref.shape
    heads = q_ref.shape[1] // HEAD_DIM
    coef = HEAD_DIM ** -0.5 * LOG2E
    lowest = jnp.finfo(jnp.float32).min
    m_ref[...] = jnp.full(m_ref.shape, lowest, jnp.float32)
    l_ref[...] = jnp.zeros(l_ref.shape, jnp.float32)
    acc_ref[...] = jnp.zeros(acc_ref.shape, jnp.float32)

    def step(j, masked):
        rows = pl.ds(pl.multiple_of(j * k_blk, k_blk), k_blk)
        keys = k_ref[rows, :]
        values = v_ref[rows, :]
        if masked:
            same = segq_ref[...] == segk_ref[order_ref[j]]
        for h in range(heads):
            q = q_ref[:, h * HEAD_DIM:(h + 1) * HEAD_DIM]
            s = lax.dot_general(q, keys, (((1,), (1,)), ((), ())), preferred_element_type=jnp.float32)
            if masked:
                s = jnp.where(same, s, lowest)
            m_old = m_ref[h]
            m_new = jnp.maximum(m_old, jnp.max(s, axis=1, keepdims=True))
            m_ref[h] = m_new
            p = jnp.exp2((s - m_new[:, :1]) * coef)
            alpha = jnp.exp2((m_old - m_new) * coef)
            part = p[:, :HEAD_DIM]
            for i in range(1, k_blk // HEAD_DIM):
                part = part + p[:, i * HEAD_DIM:(i + 1) * HEAD_DIM]
            l_ref[h] = l_ref[h] * alpha + part
            pv = jnp.dot(p.astype(jnp.bfloat16), values, preferred_element_type=jnp.float32)
            acc_ref[h] = acc_ref[h] * alpha + pv

    @pl.loop(0, n_blk)
    def _(j):
        flag = flag_ref[tile, j]

        @pl.when(flag == 1)
        def _():
            step(j, False)

        @pl.when(flag == 2)
        def _():
            step(j, True)

    for h in range(heads):
        total = jnp.sum(l_ref[h], axis=1, keepdims=True)
        o_ref[:, h * HEAD_DIM:(h + 1) * HEAD_DIM] = (acc_ref[h] / total).astype(jnp.bfloat16)


def attention(qkv, kv_all, flags, order, seg_q, seg_k):
    rows, cols = qkv.shape
    width = cols - 2 * HEAD_DIM
    heads = width // HEAD_DIM
    keys = kv_all.shape[0]
    tiles = rows // Q_TILE
    pairs = rows * heads * keys
    return pl.pallas_call(
        attention_kernel,
        out_shape=jax.ShapeDtypeStruct((rows, width), jnp.bfloat16),
        grid_spec=pltpu.PrefetchScalarGridSpec(
            num_scalar_prefetch=2,
            grid=(tiles,),
            in_specs=[
                pl.BlockSpec((Q_TILE, 1), lambda i, *_: (i, 0)),
                pl.BlockSpec(seg_k.shape, lambda i, *_: (0, 0, 0)),
                pl.BlockSpec((Q_TILE, width), lambda i, *_: (i, 0)),
                pl.BlockSpec((keys, HEAD_DIM), lambda i, *_: (0, 0)),
                pl.BlockSpec((keys, HEAD_DIM), lambda i, *_: (0, 1)),
            ],
            out_specs=pl.BlockSpec((Q_TILE, width), lambda i, *_: (i, 0)),
            scratch_shapes=[
                pltpu.VMEM((heads, Q_TILE, HEAD_DIM), jnp.float32),
                pltpu.VMEM((heads, Q_TILE, HEAD_DIM), jnp.float32),
                pltpu.VMEM((heads, Q_TILE, HEAD_DIM), jnp.float32),
            ],
        ),
        compiler_params=pltpu.CompilerParams(dimension_semantics=("arbitrary",)),
        cost_estimate=pl.CostEstimate(flops=4 * pairs * HEAD_DIM, bytes_accessed=4 * rows * cols, transcendentals=pairs),
        name="attention",
    )(flags, order, seg_q, seg_k, qkv, kv_all, kv_all)


def solution(mesh):
    n_row, n_col = mesh.shape["row"], mesh.shape["col"]
    n_x = n_row // CORES

    def near_x(x):
        return x + 1 - 2 * (x % 2)

    def far_x(x):
        return n_x - 1 - x

    core_swap = [(r, r + 1 - 2 * (r % 2)) for r in range(n_row)]
    near_swap = [(r, CORES * near_x(r // CORES) + r % CORES) for r in range(n_row)]
    far_swap = [(r, CORES * far_x(r // CORES) + r % CORES) for r in range(n_row)]
    up = [(i, (i + 1) % n_col) for i in range(n_col)]
    down = [(i, (i - 1) % n_col) for i in range(n_col)]

    def gather_col(block, panel, slot):
        half = block.shape[0] // 2
        y = lax.axis_index("col")
        before, after, across = (y - 1) % n_col, (y + 1) % n_col, (y + 2) % n_col
        top, low = block[:half], block[half:]
        top_b = lax.ppermute(top, "col", up)
        low_a = lax.ppermute(low, "col", down)
        low_b = lax.ppermute(low, "col", up)
        top_a = lax.ppermute(top, "col", down)
        top_c = lax.ppermute(top_b, "col", up)
        low_c = lax.ppermute(low_a, "col", down)
        put = lambda p, b, row, i: lax.dynamic_update_slice(p, b, (row, slot(i)))
        panel = put(panel, block, 0, y)
        panel = put(panel, top_b, 0, before)
        panel = put(panel, low_b, half, before)
        panel = put(panel, top_a, 0, after)
        panel = put(panel, low_a, half, after)
        panel = put(panel, top_c, 0, across)
        return put(panel, low_c, half, across)

    def local_block(tokens, w_qkv, w_out, doc_ids):
        rows, width = tokens.shape
        depth, cols = w_qkv.shape
        part = cols // 2
        r = lax.axis_index("row")
        x, c = r // CORES, r % CORES
        xn, xf = near_x(x), far_x(x)
        xnf = far_x(xn)
        half = x // (n_x // 2)

        seg_all = lax.all_gather(doc_ids, "row", axis=0, tiled=False)
        order = jnp.stack([CORES * a + b for b in (c, 1 - c) for a in (x, xf, xn, xnf)]).astype(jnp.int32)
        seg_par = lax.dynamic_index_in_dim(seg_all, CORES * xf + c, 0, keepdims=False)
        k_lo, k_hi = seg_all[:, 0][order], seg_all[:, -1][order]

        def tile_flags(seg):
            tiles = seg.reshape(-1, Q_TILE)
            q_lo, q_hi = tiles[:, :1], tiles[:, -1:]
            meets = (k_lo[None] <= q_hi) & (k_hi[None] >= q_lo)
            plain = (q_lo == q_hi) & (k_lo[None] == q_lo) & (k_hi[None] == q_lo)
            return jnp.where(meets, jnp.where(plain, 1, 2), 0).astype(jnp.int32)

        flags_own, flags_par = tile_flags(doc_ids), tile_flags(seg_par)
        seg_k = seg_all.reshape(n_row, 1, rows)

        tok_par = lax.ppermute(tokens, "row", far_swap)
        panel = jnp.zeros((rows, n_col * width), tokens.dtype)
        x_own = gather_col(tokens, panel, lambda i: i * width)
        x_par = gather_col(tok_par, panel, lambda i: i * width)

        keep = lax.dynamic_slice(w_qkv, (0, half * part), (depth, part))
        give = lax.dynamic_slice(w_qkv, (0, (1 - half) * part), (depth, part))
        w_near = lax.ppermute(keep, "row", near_swap)
        cut = depth // 2
        w_far = [lax.ppermute(give[:cut], "row", far_swap), lax.ppermute(give[cut:], "row", far_swap)]
        w_nf = [lax.ppermute(w, "row", near_swap) for w in w_far]
        w_full = jnp.zeros((n_row * depth, part), w_qkv.dtype)
        pieces = [(keep, x, 0), (w_near, xn, 0), (w_far[0], xf, 0), (w_far[1], xf, cut), (w_nf[0], xnf, 0), (w_nf[1], xnf, cut)]
        for piece, at, off in pieces:
            other = lax.ppermute(piece, "row", core_swap)
            w_full = lax.dynamic_update_slice(w_full, piece, ((CORES * at + c) * depth + off, 0))
            w_full = lax.dynamic_update_slice(w_full, other, ((CORES * at + 1 - c) * depth + off, 0))

        w_out, _ = lax.optimization_barrier((w_out, w_nf[1]))
        wo_full = lax.all_gather(w_out, "row", axis=0, tiled=True)

        qkv_own = jnp.dot(x_own, w_full, preferred_element_type=jnp.float32).astype(jnp.bfloat16)
        qkv_par = jnp.dot(x_par, w_full, preferred_element_type=jnp.float32).astype(jnp.bfloat16)
        ctx = part - 2 * HEAD_DIM
        kv = jnp.concatenate([qkv_own[:, ctx:], qkv_par[:, ctx:]], axis=0)
        kv = jnp.concatenate([kv, lax.ppermute(kv, "row", near_swap)], axis=0)
        kv = jnp.concatenate([kv, lax.ppermute(kv, "row", core_swap)], axis=0)

        o_par = attention(qkv_par, kv, flags_par, order, seg_par[:, None], seg_k)
        o_own = attention(qkv_own, kv, flags_own, order, doc_ids[:, None], seg_k)
        o_got = lax.ppermute(o_par, "row", far_swap)
        o_panel = jnp.zeros((rows, n_col * width), jnp.bfloat16)
        o_panel = gather_col(o_got, o_panel, lambda i: i * width + (1 - half) * ctx)
        o_panel = gather_col(o_own, o_panel, lambda i: i * width + half * ctx)
        return jnp.dot(o_panel, wo_full, preferred_element_type=jnp.float32).astype(jnp.bfloat16)

    row_spec = P(("data", "row"), "col")
    weight_spec = P("row", "col")
    return jax.shard_map(local_block, mesh=mesh, in_specs=(row_spec, weight_spec, weight_spec, P(("data", "row"))), out_specs=row_spec, check_vma=False)
```

```python
import functools

import jax
import jax.numpy as jnp
from jax import lax
from jax.experimental import pallas as pl
from jax.experimental.pallas import tpu as pltpu
from jax.sharding import PartitionSpec as P

HEAD_DIM = 128
CORES = 2
Q_TILE = 256
LOG2E = 1.4426950408889634


MESH = pl.DeviceIdType.MESH


def near_x(x):
    return x + 1 - 2 * (x % 2)


def qkv_kernel(n_x, n_y, tok_ref, w_ref, q_ref, kv_ref, xg, wg, acc, w_send, w_recv, d_send, d_recv, t_send, t_recv, y_send, y_recv, k_send, k_recv, l_sem):
    r, y = lax.axis_index("row"), lax.axis_index("col")
    x, c = r // CORES, r % CORES
    xn, xf = near_x(x), n_x - 1 - x
    xnf = n_x - 1 - xn
    half = x // (n_x // 2)
    before, after, across = (y + n_y - 1) % n_y, (y + 1) % n_y, (y + 2) % n_y
    rows, width = tok_ref.shape
    depth = w_ref.shape[0]
    part = w_ref.shape[1] // 2
    ctx = part - 2 * HEAD_DIM
    mid, cut, quarter = rows // 2, depth // 2, rows // 4
    near, far, core = {"row": CORES * xn + c}, {"row": CORES * xf + c}, {"row": CORES * x + 1 - c}
    up, down = {"col": after}, {"col": before}

    barrier = pltpu.get_barrier_semaphore()
    for peer in (near, far, core, up, down):
        pl.semaphore_signal(barrier, inc=1, device_id=peer, device_id_type=MESH)
    pl.semaphore_wait(barrier, 5)

    started = []

    def send(src, dst, s_sem, r_sem, peer):
        copy = pltpu.make_async_remote_copy(src_ref=src, dst_ref=dst, send_sem=s_sem, recv_sem=r_sem, device_id=peer, device_id_type=MESH)
        copy.start()
        started.append(copy)
        return copy

    mine = pl.ds(pl.multiple_of(half * part, 128), part)
    theirs = pl.ds(pl.multiple_of((1 - half) * part, 128), part)

    def w_slot(chip, plane, i):
        return wg.at[chip, pl.ds(pl.multiple_of(plane * depth + i * cut, cut), cut), :]

    def send_w(kind, i):
        src_rows = pl.ds(i * cut, cut)
        if kind == 0:
            return send(w_ref.at[src_rows, mine], w_slot(x, c, i), w_send.at[0, i], w_recv.at[0, i], near)
        if kind == 1:
            return send(w_ref.at[src_rows, theirs], w_slot(x, c, i), w_send.at[1, i], w_recv.at[1, i], far)
        return send(w_slot(xf, c, i), w_slot(xf, c, i), w_send.at[2, i], w_recv.at[2, i], near)

    def share(chip, i, at):
        src = w_ref.at[pl.ds(i * cut, cut), mine] if at == 0 else w_slot(chip, c, i)
        return send(src, w_slot(chip, c, i), d_send.at[at, i], d_recv.at[at, i], core)

    def x_slot(b, at, lo, n):
        return xg.at[b, at, pl.ds(lo, n), :]

    def send_t(a):
        return send(tok_ref.at[pl.ds(a * mid, mid), :], x_slot(1, y, a * mid, mid), t_send.at[a], t_recv.at[a], far)

    def send_y(b, a, way):
        src = tok_ref.at[pl.ds(a * mid, mid), :] if b == 0 else x_slot(1, y, a * mid, mid)
        return send(src, x_slot(b, y, a * mid, mid), y_send.at[b, a, way], y_recv.at[b, a, way], (up, down)[way])

    def pass_y(b, a, way):
        at = (before, after)[way]
        piece = x_slot(b, at, a * mid + way * quarter, quarter)
        return send(piece, piece, y_send.at[b, a, 2 + way], y_recv.at[b, a, 2 + way], (up, down)[way])

    w_far = [send_w(1, 0)]
    y_own = [[send_y(0, a, way) for way in (0, 1)] for a in (0, 1)]
    w_near = [send_w(0, 0)]
    tok = [send_t(0)]
    w_near.append(send_w(0, 1))
    w_far.append(send_w(1, 1))
    tok.append(send_t(1))
    locals_ = [
        pltpu.make_async_copy(tok_ref, xg.at[0, y], l_sem.at[0]),
        pltpu.make_async_copy(w_ref.at[:, mine], wg.at[x, pl.ds(pl.multiple_of(c * depth, depth), depth), :], l_sem.at[1]),
    ]
    for copy in locals_:
        copy.start()
    d_own = [share(x, i, 0) for i in (0, 1)]

    def multiply(b, lo, n, chip, first, last):
        tile = 2 * HEAD_DIM

        @pl.loop(0, part // tile)
        def _(j):
            cols = pl.ds(pl.multiple_of(j * tile, tile), tile)
            dot = jnp.dot(xg[b, chip, pl.ds(lo, n), :], wg[chip, :, cols], preferred_element_type=jnp.float32)
            if not first:
                dot = dot + acc[pl.ds(lo, n), cols]
            if not last:
                acc[pl.ds(lo, n), cols] = dot
            else:
                out = dot.astype(jnp.bfloat16)

                @pl.when(j < ctx // tile)
                def _():
                    q_ref[pl.ds(b * rows + lo, n), cols] = out

                @pl.when(j == ctx // tile)
                def _():
                    kv_ref[pl.ds(b * rows + lo, n), :] = out

    def kv_slot(s):
        return kv_ref.at[pl.ds(s * rows, rows), :]

    def kv_near(b):
        return send(kv_slot(b), kv_slot(2 + b), k_send.at[b], k_recv.at[b], near)

    def kv_core(s):
        return send(kv_slot(s), kv_slot(4 + s), k_send.at[2 + s], k_recv.at[2 + s], core)

    def relay(b, a):
        got = []
        for way in (0, 1):
            (y_own if b == 0 else y_par)[a][way].wait_recv()
            got.append(pass_y(b, a, way))
        return got

    y_far = [relay(0, 0)]
    w_far[0].wait_recv()
    w_nf = [send_w(2, 0)]
    d_far = [share(xf, 0, 2)]
    w_near[0].wait_recv()
    d_near = [share(xn, 0, 1)]
    y_far.append(relay(0, 1))
    tok[0].wait_recv()
    y_par = [[send_y(1, 0, way) for way in (0, 1)]]
    w_near[1].wait_recv()
    d_near.append(share(xn, 1, 1))
    for pair in y_far:
        for copy in pair:
            copy.wait_recv()
    for copy in locals_:
        copy.wait()
    for copy in d_own:
        copy.wait_recv()
    multiply(0, 0, rows, x, True, False)
    for copy in d_near:
        copy.wait_recv()
    w_far[1].wait_recv()
    w_nf.append(send_w(2, 1))
    d_far.append(share(xf, 1, 2))
    multiply(0, 0, rows, xn, False, False)
    w_nf[0].wait_recv()
    d_nf = [share(xnf, 0, 3)]
    y_pfar = [relay(1, 0)]
    tok[1].wait_recv()
    y_par.append([send_y(1, 1, way) for way in (0, 1)])
    for copy in d_far:
        copy.wait_recv()
    multiply(0, 0, rows, xf, False, False)
    w_nf[1].wait_recv()
    d_nf.append(share(xnf, 1, 3))
    for copy in d_nf:
        copy.wait_recv()
    multiply(0, 0, rows, xnf, False, True)
    for copy in y_pfar[0]:
        copy.wait_recv()
    multiply(1, 0, mid, y, True, False)
    k_near, k_core = [kv_near(0)], [kv_core(0)]
    multiply(1, 0, mid, before, False, False)
    y_pfar.append(relay(1, 1))
    multiply(1, 0, mid, after, False, False)
    multiply(1, 0, mid, across, False, True)
    multiply(1, mid, mid, y, True, False)
    multiply(1, mid, mid, before, False, False)
    multiply(1, mid, mid, after, False, False)
    k_near[0].wait_recv()
    k_core.append(kv_core(2))
    for copy in y_pfar[1]:
        copy.wait_recv()
    multiply(1, mid, mid, across, False, True)
    k_near.append(kv_near(1))
    k_core.append(kv_core(1))
    k_near[1].wait_recv()
    k_core.append(kv_core(3))
    for copy in k_core:
        copy.wait_recv()
    for copy in started:
        copy.wait_send()


def project_qkv(tokens, w_qkv, n_x, n_y):
    rows, width = tokens.shape
    depth, cols = w_qkv.shape
    part = cols // 2
    ctx = part - 2 * HEAD_DIM
    dma = pltpu.SemaphoreType.DMA
    return pl.pallas_call(
        functools.partial(qkv_kernel, n_x, n_y),
        out_shape=(jax.ShapeDtypeStruct((2 * rows, ctx), jnp.bfloat16), jax.ShapeDtypeStruct((CORES * n_x * rows, 2 * HEAD_DIM), jnp.bfloat16)),
        in_specs=[pl.BlockSpec(memory_space=pl.ANY)] * 2,
        out_specs=(pl.BlockSpec(memory_space=pltpu.VMEM),) * 2,
        scratch_shapes=[
            pltpu.VMEM((2, n_y, rows, width), jnp.bfloat16),
            pltpu.VMEM((n_x, CORES * depth, part), jnp.bfloat16),
            pltpu.VMEM((rows, part), jnp.float32),
            dma((3, 2)), dma((3, 2)), dma((4, 2)), dma((4, 2)), dma((2,)), dma((2,)),
            dma((2, 2, 4)), dma((2, 2, 4)), dma((6,)), dma((6,)), dma((2,)),
        ],
        compiler_params=pltpu.CompilerParams(collective_id=0, has_side_effects=True, vmem_limit_bytes=60 * 1024 * 1024),
        cost_estimate=pl.CostEstimate(flops=4 * rows * n_y * width * part, bytes_accessed=2 * depth * cols, transcendentals=0),
        name="project_qkv",
    )(tokens, w_qkv)


def attention_kernel(flag_ref, order_ref, segq_ref, segk_ref, q_ref, k_ref, v_ref, o_ref, m_ref, l_ref, acc_ref):
    tile = pl.program_id(0)
    n_blk, _, k_blk = segk_ref.shape
    heads = q_ref.shape[1] // HEAD_DIM
    coef = HEAD_DIM ** -0.5 * LOG2E
    lowest = jnp.finfo(jnp.float32).min
    m_ref[...] = jnp.full(m_ref.shape, lowest, jnp.float32)
    l_ref[...] = jnp.zeros(l_ref.shape, jnp.float32)
    acc_ref[...] = jnp.zeros(acc_ref.shape, jnp.float32)

    def step(j, masked):
        rows = pl.ds(pl.multiple_of(j * k_blk, k_blk), k_blk)
        keys = k_ref[rows, :]
        values = v_ref[rows, :]
        if masked:
            same = segq_ref[...] == segk_ref[order_ref[j]]
        for h in range(heads):
            q = q_ref[:, h * HEAD_DIM:(h + 1) * HEAD_DIM]
            s = lax.dot_general(q, keys, (((1,), (1,)), ((), ())), preferred_element_type=jnp.float32)
            if masked:
                s = jnp.where(same, s, lowest)
            m_old = m_ref[h]
            m_new = jnp.maximum(m_old, jnp.max(s, axis=1, keepdims=True))
            m_ref[h] = m_new
            p = jnp.exp2((s - m_new[:, :1]) * coef)
            alpha = jnp.exp2((m_old - m_new) * coef)
            part = p[:, :HEAD_DIM]
            for i in range(1, k_blk // HEAD_DIM):
                part = part + p[:, i * HEAD_DIM:(i + 1) * HEAD_DIM]
            l_ref[h] = l_ref[h] * alpha + part
            pv = jnp.dot(p.astype(jnp.bfloat16), values, preferred_element_type=jnp.float32)
            acc_ref[h] = acc_ref[h] * alpha + pv

    @pl.loop(0, n_blk)
    def _(j):
        flag = flag_ref[tile, j]

        @pl.when(flag == 1)
        def _():
            step(j, False)

        @pl.when(flag == 2)
        def _():
            step(j, True)

    for h in range(heads):
        total = jnp.sum(l_ref[h], axis=1, keepdims=True)
        o_ref[:, h * HEAD_DIM:(h + 1) * HEAD_DIM] = (acc_ref[h] / total).astype(jnp.bfloat16)


def attention(q_all, base, kv_all, flags, order, seg_q, seg_k):
    rows, width = seg_q.shape[0], q_all.shape[1]
    heads = width // HEAD_DIM
    keys = kv_all.shape[0]
    tiles = rows // Q_TILE
    pairs = rows * heads * keys
    return pl.pallas_call(
        attention_kernel,
        out_shape=jax.ShapeDtypeStruct((rows, width), jnp.bfloat16),
        grid_spec=pltpu.PrefetchScalarGridSpec(
            num_scalar_prefetch=2,
            grid=(tiles,),
            in_specs=[
                pl.BlockSpec((Q_TILE, 1), lambda i, *_: (i, 0)),
                pl.BlockSpec(seg_k.shape, lambda i, *_: (0, 0, 0)),
                pl.BlockSpec((Q_TILE, width), lambda i, *_: (base * tiles + i, 0)),
                pl.BlockSpec((keys, HEAD_DIM), lambda i, *_: (0, 0)),
                pl.BlockSpec((keys, HEAD_DIM), lambda i, *_: (0, 1)),
            ],
            out_specs=pl.BlockSpec((Q_TILE, width), lambda i, *_: (i, 0)),
            scratch_shapes=[
                pltpu.VMEM((heads, Q_TILE, HEAD_DIM), jnp.float32),
                pltpu.VMEM((heads, Q_TILE, HEAD_DIM), jnp.float32),
                pltpu.VMEM((heads, Q_TILE, HEAD_DIM), jnp.float32),
            ],
        ),
        compiler_params=pltpu.CompilerParams(dimension_semantics=("arbitrary",)),
        cost_estimate=pl.CostEstimate(flops=4 * pairs * HEAD_DIM, bytes_accessed=4 * rows * width, transcendentals=pairs),
        name="attention",
    )(flags, order, seg_q, seg_k, q_all, kv_all, kv_all)


def solution(mesh):
    n_row, n_col = mesh.shape["row"], mesh.shape["col"]
    n_x = n_row // CORES

    def far_x(x):
        return n_x - 1 - x

    far_swap = [(r, CORES * far_x(r // CORES) + r % CORES) for r in range(n_row)]
    up = [(i, (i + 1) % n_col) for i in range(n_col)]
    down = [(i, (i - 1) % n_col) for i in range(n_col)]

    def gather_col(block, panel, slot):
        half = block.shape[0] // 2
        y = lax.axis_index("col")
        before, after, across = (y - 1) % n_col, (y + 1) % n_col, (y + 2) % n_col
        top, low = block[:half], block[half:]
        top_b = lax.ppermute(top, "col", up)
        low_a = lax.ppermute(low, "col", down)
        low_b = lax.ppermute(low, "col", up)
        top_a = lax.ppermute(top, "col", down)
        top_c = lax.ppermute(top_b, "col", up)
        low_c = lax.ppermute(low_a, "col", down)
        put = lambda p, b, row, i: lax.dynamic_update_slice(p, b, (row, slot(i)))
        panel = put(panel, block, 0, y)
        panel = put(panel, top_b, 0, before)
        panel = put(panel, low_b, half, before)
        panel = put(panel, top_a, 0, after)
        panel = put(panel, low_a, half, after)
        panel = put(panel, top_c, 0, across)
        return put(panel, low_c, half, across)

    def local_block(tokens, w_qkv, w_out, doc_ids):
        rows, width = tokens.shape
        r = lax.axis_index("row")
        x, c = r // CORES, r % CORES
        xn, xf = near_x(x), far_x(x)
        xnf = far_x(xn)
        half = x // (n_x // 2)

        seg_all = lax.all_gather(doc_ids, "row", axis=0, tiled=False)
        order = jnp.stack([CORES * a + b for b in (c, 1 - c) for a in (x, xf, xn, xnf)]).astype(jnp.int32)
        seg_par = lax.dynamic_index_in_dim(seg_all, CORES * xf + c, 0, keepdims=False)
        k_lo, k_hi = seg_all[:, 0][order], seg_all[:, -1][order]

        def tile_flags(seg):
            tiles = seg.reshape(-1, Q_TILE)
            q_lo, q_hi = tiles[:, :1], tiles[:, -1:]
            meets = (k_lo[None] <= q_hi) & (k_hi[None] >= q_lo)
            plain = (q_lo == q_hi) & (k_lo[None] == q_lo) & (k_hi[None] == q_lo)
            return jnp.where(meets, jnp.where(plain, 1, 2), 0).astype(jnp.int32)

        flags_own, flags_par = tile_flags(doc_ids), tile_flags(seg_par)
        seg_k = seg_all.reshape(n_row, 1, rows)

        q_all, kv = project_qkv(tokens, w_qkv, n_x, n_col)
        ctx = q_all.shape[1]
        w_out, q_all = lax.optimization_barrier((w_out, q_all))
        wo_full = lax.all_gather(w_out, "row", axis=0, tiled=True)

        o_par = attention(q_all, 1, kv, flags_par, order, seg_par[:, None], seg_k)
        o_own = attention(q_all, 0, kv, flags_own, order, doc_ids[:, None], seg_k)
        o_got = lax.ppermute(o_par, "row", far_swap)
        o_panel = jnp.zeros((rows, n_col * width), jnp.bfloat16)
        o_panel = gather_col(o_got, o_panel, lambda i: i * width + (1 - half) * ctx)
        o_panel = gather_col(o_own, o_panel, lambda i: i * width + half * ctx)
        return jnp.dot(o_panel, wo_full, preferred_element_type=jnp.float32).astype(jnp.bfloat16)

    row_spec = P(("data", "row"), "col")
    weight_spec = P("row", "col")
    return jax.shard_map(local_block, mesh=mesh, in_specs=(row_spec, weight_spec, weight_spec, P(("data", "row"))), out_specs=row_spec, check_vma=False)
```

```python
import functools

import jax
import jax.numpy as jnp
from jax import lax
from jax.experimental import pallas as pl
from jax.experimental.pallas import tpu as pltpu
from jax.sharding import PartitionSpec as P

HEAD_DIM = 128
CORES = 2
Q_TILE = 256
CHUNKS = 4
LOG2E = 1.4426950408889634
BOTH = (0, 1)
YES, NO = True, False


MESH = pl.DeviceIdType.MESH


def near_x(x):
    return x + 1 - 2 * (x % 2)


def qkv_kernel(n_x, n_y, tok_ref, w_ref, wo_ref, seg_ref, q_ref, kv_ref, segs_ref, got_ref, xg, wg, acc, w_send, w_recv, d_send, d_recv, t_send, t_recv, y_send, y_recv, k_send, k_recv, l_sem, s_send, s_recv, o_send, o_recv):
    r, y = lax.axis_index("row"), lax.axis_index("col")
    x, c = r // CORES, r % CORES
    xn, xf = near_x(x), n_x - 1 - x
    xnf = n_x - 1 - xn
    half = x // (n_x // 2)
    before, after, across = (y + n_y - 1) % n_y, (y + 1) % n_y, (y + 2) % n_y
    rows, width = tok_ref.shape
    depth = w_ref.shape[0]
    part = w_ref.shape[1] // 2
    ctx = part - 2 * HEAD_DIM
    mid, cut, quarter = rows // 2, depth // 2, rows // 4
    near, far, core = {"row": CORES * xn + c}, {"row": CORES * xf + c}, {"row": CORES * x + 1 - c}
    up, down = {"col": after}, {"col": before}

    barrier = pltpu.get_barrier_semaphore()
    n_row = CORES * n_x
    row_peers = [{"row": (r + d) % n_row} for d in range(1, n_row)]
    for peer in row_peers + [up, down]:
        pl.semaphore_signal(barrier, inc=1, device_id=peer, device_id_type=MESH)
    pl.semaphore_wait(barrier, n_row + 1)

    started = []

    def send(src, dst, s_sem, r_sem, peer):
        copy = pltpu.make_async_remote_copy(src_ref=src, dst_ref=dst, send_sem=s_sem, recv_sem=r_sem, device_id=peer, device_id_type=MESH)
        copy.start()
        started.append(copy)
        return copy

    mine = pl.ds(pl.multiple_of(half * part, 128), part)
    theirs = pl.ds(pl.multiple_of((1 - half) * part, 128), part)

    def w_slot(chip, plane, i):
        return wg.at[chip, pl.ds(pl.multiple_of(plane * depth + i * cut, cut), cut), :]

    def send_w(kind, i):
        src_rows = pl.ds(i * cut, cut)
        if kind == 0:
            return send(w_ref.at[src_rows, mine], w_slot(x, c, i), w_send.at[0, i], w_recv.at[0, i], near)
        if kind == 1:
            return send(w_ref.at[src_rows, theirs], w_slot(x, c, i), w_send.at[1, i], w_recv.at[1, i], far)
        return send(w_slot(xf, c, i), w_slot(xf, c, i), w_send.at[2, i], w_recv.at[2, i], near)

    def share(chip, i, at):
        src = w_ref.at[pl.ds(i * cut, cut), mine] if at == 0 else w_slot(chip, c, i)
        return send(src, w_slot(chip, c, i), d_send.at[at, i], d_recv.at[at, i], core)

    def x_slot(b, at, lo, n):
        return xg.at[b, at, pl.ds(lo, n), :]

    def send_t(a):
        return send(tok_ref.at[pl.ds(a * mid, mid), :], x_slot(1, y, a * mid, mid), t_send.at[a], t_recv.at[a], far)

    def send_y(b, a, way):
        src = tok_ref.at[pl.ds(a * mid, mid), :] if b == 0 else x_slot(1, y, a * mid, mid)
        return send(src, x_slot(b, y, a * mid, mid), y_send.at[b, a, way], y_recv.at[b, a, way], (up, down)[way])

    def pass_y(b, a, way):
        at = (before, after)[way]
        piece = x_slot(b, at, a * mid + way * quarter, quarter)
        return send(piece, piece, y_send.at[b, a, 2 + way], y_recv.at[b, a, 2 + way], (up, down)[way])

    segs = [send(seg_ref, segs_ref.at[r], s_send.at[d], s_recv.at[d], peer) for d, peer in enumerate(row_peers)]
    w_far = [send_w(1, 0)]
    y_own = [[send_y(0, a, way) for way in BOTH] for a in BOTH]
    w_near = [send_w(0, 0)]
    tok = [send_t(0)]
    w_near.append(send_w(0, 1))
    w_far.append(send_w(1, 1))
    tok.append(send_t(1))
    chunk = depth // CHUNKS
    wo_got = [send(wo_ref.at[pl.ds(i * chunk, chunk), :], got_ref.at[1 + i], o_send.at[1 + i], o_recv.at[1 + i], far) for i in BOTH]
    locals_ = [
        pltpu.make_async_copy(seg_ref, segs_ref.at[r], l_sem.at[2]),
        pltpu.make_async_copy(tok_ref, xg.at[0, y], l_sem.at[0]),
        pltpu.make_async_copy(w_ref.at[:, mine], wg.at[x, pl.ds(pl.multiple_of(c * depth, depth), depth), :], l_sem.at[1]),
    ]
    for copy in locals_:
        copy.start()
    d_own = [share(x, i, 0) for i in BOTH]

    def multiply(b, lo, n, chip, first, last):
        tile = 2 * HEAD_DIM

        @pl.loop(0, part // tile)
        def _(j):
            cols = pl.ds(pl.multiple_of(j * tile, tile), tile)
            dot = jnp.dot(xg[b, chip, pl.ds(lo, n), :], wg[chip, :, cols], preferred_element_type=jnp.float32)
            if not first:
                dot = dot + acc[pl.ds(lo, n), cols]
            if not last:
                acc[pl.ds(lo, n), cols] = dot
            else:
                out = dot.astype(jnp.bfloat16)

                @pl.when(j < ctx // tile)
                def _():
                    q_ref[pl.ds(b * rows + lo, n), cols] = out

                @pl.when(j == ctx // tile)
                def _():
                    kv_ref[pl.ds(b * rows + lo, n), :] = out

    def kv_slot(s):
        return kv_ref.at[pl.ds(s * rows, rows), :]

    def kv_near(b):
        return send(kv_slot(b), kv_slot(2 + b), k_send.at[b], k_recv.at[b], near)

    def kv_core(s):
        return send(kv_slot(s), kv_slot(4 + s), k_send.at[2 + s], k_recv.at[2 + s], core)

    def relay(b, a):
        got = []
        for way in BOTH:
            (y_own if b == 0 else y_par)[a][way].wait_recv()
            got.append(pass_y(b, a, way))
        return got

    y_far = [relay(0, 0)]
    w_far[0].wait_recv()
    w_nf = [send_w(2, 0)]
    d_far = [share(xf, 0, 2)]
    w_near[0].wait_recv()
    d_near = [share(xn, 0, 1)]
    y_far.append(relay(0, 1))
    tok[0].wait_recv()
    y_par = [[send_y(1, 0, way) for way in BOTH]]
    w_near[1].wait_recv()
    d_near.append(share(xn, 1, 1))
    for pair in y_far:
        for copy in pair:
            copy.wait_recv()
    for copy in locals_:
        copy.wait()
    for copy in d_own:
        copy.wait_recv()
    multiply(0, 0, rows, x, YES, NO)
    for copy in d_near:
        copy.wait_recv()
    w_far[1].wait_recv()
    w_nf.append(send_w(2, 1))
    wo_got.append(send(wo_ref.at[pl.ds(0, chunk), :], got_ref.at[0], o_send.at[0], o_recv.at[0], near))
    d_far.append(share(xf, 1, 2))
    multiply(0, 0, rows, xn, NO, NO)
    w_nf[0].wait_recv()
    d_nf = [share(xnf, 0, 3)]
    y_pfar = [relay(1, 0)]
    tok[1].wait_recv()
    y_par.append([send_y(1, 1, way) for way in BOTH])
    for copy in d_far:
        copy.wait_recv()
    multiply(0, 0, rows, xf, NO, NO)
    w_nf[1].wait_recv()
    d_nf.append(share(xnf, 1, 3))
    for copy in d_nf:
        copy.wait_recv()
    multiply(0, 0, rows, xnf, NO, YES)
    for copy in y_pfar[0]:
        copy.wait_recv()
    multiply(1, 0, mid, y, YES, NO)
    k_near, k_core = [kv_near(0)], [kv_core(0)]
    multiply(1, 0, mid, before, NO, NO)
    y_pfar.append(relay(1, 1))
    multiply(1, 0, mid, after, NO, NO)
    multiply(1, 0, mid, across, NO, YES)
    multiply(1, mid, mid, y, YES, NO)
    multiply(1, mid, mid, before, NO, NO)
    multiply(1, mid, mid, after, NO, NO)
    k_near[0].wait_recv()
    k_core.append(kv_core(2))
    for copy in y_pfar[1]:
        copy.wait_recv()
    multiply(1, mid, mid, across, NO, YES)
    k_near.append(kv_near(1))
    k_core.append(kv_core(1))
    k_near[1].wait_recv()
    k_core.append(kv_core(3))
    for copy in k_core + wo_got + segs:
        copy.wait_recv()
    for copy in started:
        copy.wait_send()


def project_qkv(tokens, w_qkv, w_out, doc_ids, n_x, n_y):
    rows, width = tokens.shape
    depth, cols = w_qkv.shape
    part = cols // 2
    ctx = part - 2 * HEAD_DIM
    n_row = CORES * n_x
    dma = pltpu.SemaphoreType.DMA
    anywhere, vmem = pl.BlockSpec(memory_space=pl.ANY), pl.BlockSpec(memory_space=pltpu.VMEM)
    segs = doc_ids.reshape(rows // 128, 128)
    return pl.pallas_call(
        functools.partial(qkv_kernel, n_x, n_y),
        out_shape=(
            jax.ShapeDtypeStruct((2 * rows, ctx), jnp.bfloat16),
            jax.ShapeDtypeStruct((n_row * rows, 2 * HEAD_DIM), jnp.bfloat16),
            jax.ShapeDtypeStruct((n_row,) + segs.shape, jnp.int32),
            jax.ShapeDtypeStruct((3, depth // CHUNKS, w_out.shape[1]), jnp.bfloat16),
        ),
        in_specs=[anywhere] * 4,
        out_specs=(vmem, vmem, vmem, anywhere),
        scratch_shapes=[
            pltpu.VMEM((2, n_y, rows, width), jnp.bfloat16),
            pltpu.VMEM((n_x, CORES * depth, part), jnp.bfloat16),
            pltpu.VMEM((rows, part), jnp.float32),
            dma((3, 2)), dma((3, 2)), dma((4, 2)), dma((4, 2)), dma((2,)), dma((2,)),
            dma((2, 2, 4)), dma((2, 2, 4)), dma((6,)), dma((6,)), dma((3,)),
            dma((n_row - 1,)), dma((n_row - 1,)), dma((3,)), dma((3,)),
        ],
        compiler_params=pltpu.CompilerParams(collective_id=0, has_side_effects=YES, vmem_limit_bytes=60 * 1024 * 1024),
        cost_estimate=pl.CostEstimate(flops=4 * rows * n_y * width * part, bytes_accessed=2 * depth * cols, transcendentals=0),
        name="project_qkv",
    )(tokens, w_qkv, w_out, segs)


def attend_kernel(n_x, n_y, q_ref, kv_ref, segs_ref, got_ref, w_ref, out_ref, wo, panel, obuf, sbuf, segq, mbuf, lbuf, abuf, n_send, n_recv, f_send, f_recv, d_send, d_recv, t_send, t_recv, y_send, y_recv, l_sem):
    r, y = lax.axis_index("row"), lax.axis_index("col")
    x, c = r // CORES, r % CORES
    xn, xf = near_x(x), n_x - 1 - x
    xnf = n_x - 1 - xn
    half = x // (n_x // 2)
    before, after, across = (y + n_y - 1) % n_y, (y + 1) % n_y, (y + 2) % n_y
    rows = out_ref.shape[0]
    keys = kv_ref.shape[0]
    chunk = w_ref.shape[0] // CHUNKS
    width = w_ref.shape[1]
    heads = q_ref.shape[1] // HEAD_DIM
    tiles = 2 * rows // Q_TILE
    units = tiles * heads
    eighth = Q_TILE // 2
    coef = HEAD_DIM ** -0.5 * LOG2E
    lowest = jnp.finfo(jnp.float32).min
    near, far, core = {"row": CORES * xn + c}, {"row": CORES * xf + c}, {"row": CORES * x + 1 - c}
    up, down = {"col": after}, {"col": before}

    barrier = pltpu.get_barrier_semaphore()
    for peer in (near, far, core, up, down):
        pl.semaphore_signal(barrier, inc=1, device_id=peer, device_id_type=MESH)
    pl.semaphore_wait(barrier, 5)

    started = []

    def send(src, dst, s_sem, r_sem, peer):
        copy = pltpu.make_async_remote_copy(src_ref=src, dst_ref=dst, send_sem=s_sem, recv_sem=r_sem, device_id=peer, device_id_type=MESH)
        copy.start()
        started.append(copy)
        return copy

    def w_slot(k, chip):
        return wo.at[k, pl.ds(pl.multiple_of((CORES * chip + c) * chunk, chunk), chunk), :]

    def w_mine(k):
        return w_ref.at[pl.ds(k * chunk, chunk), :]

    def share(k, origin, src=None):
        slot = w_slot(k, (x, xn, xf, xnf)[origin])
        return send(slot if src is None else src, slot, d_send.at[k, origin], d_recv.at[k, origin], core)

    def to_near(k, src, chip):
        return send(src, w_slot(k, chip), n_send.at[k, 0], n_recv.at[k, 0], near)

    def to_far(k, src, chip):
        return send(src, w_slot(k, chip), f_send.at[k, 0], f_recv.at[k, 0], far)

    direct = {2: to_near(2, w_mine(2), x), 3: to_near(3, w_mine(3), x)}
    straight = {2: to_far(2, w_mine(2), x), 3: to_far(3, w_mine(3), x)}
    direct[1] = to_near(1, w_mine(1), x)
    corner = {0: send(got_ref.at[1], w_slot(0, xf), n_send.at[0, 1], n_recv.at[0, 1], near)}
    corner[1] = send(got_ref.at[2], w_slot(1, xf), n_send.at[1, 1], n_recv.at[1, 1], near)
    places = [(w_mine(k), w_slot(k, x)) for k in range(CHUNKS)]
    places += [(got_ref.at[0], w_slot(0, xn)), (got_ref.at[1], w_slot(0, xf)), (got_ref.at[2], w_slot(1, xf))]
    placed = [pltpu.make_async_copy(src, dst, l_sem.at[i]) for i, (src, dst) in enumerate(places)]
    for copy in placed:
        copy.start()
    shared = [share(k, 0, w_mine(k)) for k in range(CHUNKS)]
    shared += [share(0, 1, got_ref.at[0]), share(0, 2, got_ref.at[1]), share(1, 2, got_ref.at[2])]

    for i in range(2 * rows // 128):
        at = r if i < rows // 128 else CORES * xf + c
        line = segs_ref[at, pl.ds(i % (rows // 128), 1), :].astype(jnp.float32)
        segq[pl.ds(i * 128, 128), :] = jnp.broadcast_to(line, (128, 128)).T

    def key_row(j):
        odd, fam, plane = j % 2, (j // 2) % 2, j // 4
        base = x + fam * (xn - x)
        chip = base + odd * (n_x - 1 - 2 * base)
        return CORES * chip + c + plane * (1 - 2 * c)

    blocks = keys // rows
    lanes = rows // 128

    def scores(u, j):
        b, tile, h = u % 3, u // heads, u % heads
        q = q_ref[pl.ds(pl.multiple_of(tile * Q_TILE, Q_TILE), Q_TILE), pl.ds(pl.multiple_of(h * HEAD_DIM, HEAD_DIM), HEAD_DIM)]
        k = kv_ref[pl.ds(pl.multiple_of(j * rows, rows), rows), pl.ds(0, HEAD_DIM)]
        s = lax.dot_general(q, k, (((1,), (1,)), ((), ())), preferred_element_type=jnp.float32)
        own = segq[pl.ds(pl.multiple_of(tile * Q_TILE, Q_TILE), Q_TILE), :]
        seg = segs_ref[key_row(j)].astype(jnp.float32)
        top = mbuf[b]
        for i in range(lanes):
            part = jnp.where(own == seg[i:i + 1, :], s[:, i * 128:(i + 1) * 128], lowest)
            sbuf[b, j * lanes + i] = part
            top = jnp.maximum(top, part)
        mbuf[b] = top

    def powers(u, j):
        b = u % 3
        top = mbuf[b]
        total = lbuf[b]
        for i in range(lanes):
            e = jnp.exp2((sbuf[b, j * lanes + i] - top) * coef)
            sbuf[b, j * lanes + i] = e
            total = total + e
        lbuf[b] = total

    def context(u, j):
        b = u % 3
        inv = lbuf[b]
        p = jnp.concatenate([(sbuf[b, j * lanes + i] * inv).astype(jnp.bfloat16) for i in range(lanes)], axis=1)
        v = kv_ref[pl.ds(pl.multiple_of(j * rows, rows), rows), pl.ds(HEAD_DIM, HEAD_DIM)]
        abuf[...] += jnp.dot(p, v, preferred_element_type=jnp.float32)

    def open_unit(u, a, b, e):
        if a:
            mbuf[u % 3] = jnp.full(mbuf.shape[1:], lowest, jnp.float32)
        if b:
            lbuf[(u - 1) % 3] = jnp.zeros(lbuf.shape[1:], jnp.float32)
        if e:
            abuf[...] = jnp.zeros(abuf.shape, jnp.float32)

    def close_unit(u, a, b, e):
        if a:
            mbuf[u % 3] = jnp.broadcast_to(jnp.max(mbuf[u % 3], axis=1, keepdims=YES), mbuf.shape[1:])
        if b:
            lbuf[(u - 1) % 3] = 1.0 / jnp.broadcast_to(jnp.sum(lbuf[(u - 1) % 3], axis=1, keepdims=YES), lbuf.shape[1:])
        if e:
            tile, h = (u - 2) // heads, (u - 2) % heads
            out = abuf[...].astype(jnp.bfloat16)
            per = heads // CHUNKS
            lo = pl.multiple_of((h % per) * HEAD_DIM, HEAD_DIM)
            mine = pl.multiple_of((CORES * y + half) * chunk, chunk)

            @pl.when(tile < tiles // 2)
            def _():
                panel[h // per, pl.ds(pl.multiple_of(tile * Q_TILE, Q_TILE), Q_TILE), pl.ds(pl.multiple_of(mine + lo, HEAD_DIM), HEAD_DIM)] = out

            @pl.when(tile >= tiles // 2)
            def _():
                obuf[h // per, pl.ds(pl.multiple_of((tile - tiles // 2) * Q_TILE, Q_TILE), Q_TILE), pl.ds(lo, HEAD_DIM)] = out

    def unit(u, a, b, e):
        open_unit(u, a, b, e)

        @pl.loop(0, blocks)
        def _(j):
            if a:
                scores(u, j)
            if b:
                powers(u - 1, j)
            if e:
                context(u - 2, j)

        close_unit(u, a, b, e)

    def o_slot(yy, f, lo, n):
        hh = half + f * (1 - 2 * half)
        return panel.at[:, pl.ds(lo, n), pl.ds(pl.multiple_of((CORES * yy + hh) * chunk, chunk), chunk)]

    def send_o(a):
        return pltpu.make_async_remote_copy(
            src_ref=obuf.at[:, pl.ds(a * Q_TILE, Q_TILE), :], dst_ref=o_slot(y, 0, a * Q_TILE, Q_TILE),
            send_sem=t_send.at[a], recv_sem=t_recv.at[a], device_id=far, device_id_type=MESH)

    def y_copy(f, a, way):
        piece = o_slot(y, f, a * Q_TILE, Q_TILE)
        return pltpu.make_async_remote_copy(src_ref=piece, dst_ref=piece, send_sem=y_send.at[f, a, way], recv_sem=y_recv.at[f, a, way], device_id=(up, down)[way], device_id_type=MESH)

    def y_pass(f, a, way):
        piece = o_slot((before, after)[way], f, a * Q_TILE + way * eighth, eighth)
        return pltpu.make_async_remote_copy(src_ref=piece, dst_ref=piece, send_sem=y_send.at[f, a, 2 + way], recv_sem=y_recv.at[f, a, 2 + way], device_id=(up, down)[way], device_id_type=MESH)

    def w_copy(kind, k):
        if kind == 0:
            return pltpu.make_async_remote_copy(src_ref=w_slot(k, xn), dst_ref=w_slot(k, xn), send_sem=f_send.at[k, 1], recv_sem=f_recv.at[k, 1], device_id=far, device_id_type=MESH)
        slot = w_slot(k, (x, xn, xf, xnf)[kind])
        return pltpu.make_async_remote_copy(src_ref=slot, dst_ref=slot, send_sem=d_send.at[k, kind], recv_sem=d_recv.at[k, kind], device_id=core, device_id_type=MESH)

    def near_in(k):
        direct[k].wait_recv()
        if k >= 2:
            w_copy(0, k).start()
        w_copy(1, k).start()

    def far_in(k):
        straight[k].wait_recv()
        w_copy(2, k).start()

    def corner_in(k):
        (corner[k] if k < 2 else w_copy(0, k)).wait_recv()
        w_copy(3, k).start()

    def y_start(f, a):
        for way in BOTH:
            y_copy(f, a, way).start()

    def y_relay(f, a):
        for way in BOTH:
            y_copy(f, a, way).wait_recv()
            y_pass(f, a, way).start()

    def o_in(a):
        send_o(a).wait_recv()
        y_start(1, a)

    events = {
        heads + 3: [lambda: y_start(0, 0), lambda: near_in(2), lambda: far_in(2)],
        2 * heads + 3: [lambda: y_start(0, 1), lambda: y_relay(0, 0)],
        2 * heads + 6: [lambda: near_in(3), lambda: far_in(3)],
        3 * heads + 1: [lambda: y_relay(0, 1)],
        3 * heads + 3: [lambda: send_o(0).start()],
        4 * heads - 1: [lambda: corner_in(2)],
    }

    unit(0, YES, NO, NO)
    unit(1, YES, YES, NO)

    @pl.loop(2, units)
    def _(u):
        for at, steps in events.items():
            @pl.when(u == at)
            def _(steps=steps):
                for step in steps:
                    step()
        unit(u, YES, YES, YES)

    unit(units, NO, YES, YES)
    unit(units + 1, NO, NO, YES)

    def multiply(a, k, first, last):
        tile = 2 * HEAD_DIM

        @pl.loop(0, width // tile)
        def _(n):
            cols = pl.ds(pl.multiple_of(n * tile, tile), tile)
            dot = jnp.dot(panel[k, pl.ds(a * Q_TILE, Q_TILE), :], wo[k, :, cols], preferred_element_type=jnp.float32)
            per = tile // 128
            if not first:
                dot = dot + jnp.concatenate([sbuf[a, n * per + i] for i in range(per)], axis=1)
            if not last:
                for i in range(per):
                    sbuf[a, n * per + i] = dot[:, i * 128:(i + 1) * 128]
            else:
                out_ref[pl.ds(a * Q_TILE, Q_TILE), cols] = dot.astype(jnp.bfloat16)

    o_in(0)
    send_o(1).start()
    corner_in(0)
    near_in(1)
    y_relay(1, 0)
    o_in(1)
    for f in BOTH:
        for way in BOTH:
            y_pass(f, 0, way).wait_recv()
    for copy in placed:
        copy.wait()
    for copy in shared:
        copy.wait_recv()
    for kind in (1, 2, 3):
        w_copy(kind, 2).wait_recv()
    multiply(0, 2, YES, NO)
    corner_in(3)
    y_relay(1, 1)
    w_copy(3, 0).wait_recv()
    multiply(0, 0, NO, NO)
    for kind in (1, 2, 3):
        w_copy(kind, 3).wait_recv()
    multiply(0, 3, NO, NO)
    for f in BOTH:
        for way in BOTH:
            y_pass(f, 1, way).wait_recv()
    multiply(1, 2, YES, NO)
    corner_in(1)
    multiply(1, 0, NO, NO)
    multiply(1, 3, NO, NO)
    w_copy(1, 1).wait_recv()
    w_copy(3, 1).wait_recv()
    multiply(0, 1, NO, YES)
    multiply(1, 1, NO, YES)
    for copy in started:
        copy.wait_send()
    for k in (2, 3):
        w_copy(0, k).wait_send()
        for kind in (1, 2, 3):
            w_copy(kind, k).wait_send()
    for kind, k in ((3, 0), (1, 1), (3, 1)):
        w_copy(kind, k).wait_send()
    for a in BOTH:
        send_o(a).wait_send()
        for f in BOTH:
            for way in BOTH:
                y_copy(f, a, way).wait_send()
                y_pass(f, a, way).wait_send()


def attend_project(q, kv, segs, got, w_out, n_x, n_y):
    rows, ctx = q.shape[0] // 2, q.shape[1]
    keys = kv.shape[0]
    depth, width = w_out.shape
    n_row = CORES * n_x
    chunk = depth // CHUNKS
    dma = pltpu.SemaphoreType.DMA
    anywhere, vmem = pl.BlockSpec(memory_space=pl.ANY), pl.BlockSpec(memory_space=pltpu.VMEM)
    return pl.pallas_call(
        functools.partial(attend_kernel, n_x, n_y),
        out_shape=jax.ShapeDtypeStruct((rows, width), jnp.bfloat16),
        in_specs=[vmem, vmem, vmem, anywhere, anywhere],
        out_specs=vmem,
        scratch_shapes=[
            pltpu.VMEM((CHUNKS, n_row * chunk, width), jnp.bfloat16),
            pltpu.VMEM((CHUNKS, rows, n_row * chunk), jnp.bfloat16),
            pltpu.VMEM((CHUNKS, rows, chunk), jnp.bfloat16),
            pltpu.VMEM((3, keys // 128, Q_TILE, 128), jnp.float32),
            pltpu.VMEM((2 * rows, 128), jnp.float32),
            pltpu.VMEM((3, Q_TILE, 128), jnp.float32),
            pltpu.VMEM((3, Q_TILE, 128), jnp.float32),
            pltpu.VMEM((Q_TILE, HEAD_DIM), jnp.float32),
            dma((CHUNKS, 2)), dma((CHUNKS, 2)), dma((CHUNKS, 2)), dma((CHUNKS, 2)),
            dma((CHUNKS, 4)), dma((CHUNKS, 4)), dma((2,)), dma((2,)),
            dma((2, 2, 4)), dma((2, 2, 4)), dma((CHUNKS + 3,)),
        ],
        compiler_params=pltpu.CompilerParams(collective_id=1, has_side_effects=YES, vmem_limit_bytes=63 * 1024 * 1024),
        cost_estimate=pl.CostEstimate(flops=8 * rows * ctx * keys, bytes_accessed=4 * depth * width, transcendentals=0),
        name="attend_project",
    )(q, kv, segs, got, w_out)


def solution(mesh):
    n_x, n_y = mesh.shape["row"] // CORES, mesh.shape["col"]

    def local_block(tokens, w_qkv, w_out, doc_ids):
        q, kv, segs, got = project_qkv(tokens, w_qkv, w_out, doc_ids, n_x, n_y)
        return attend_project(q, kv, segs, got, w_out, n_x, n_y)

    row_spec = P(("data", "row"), "col")
    weight_spec = P("row", "col")
    return jax.shard_map(local_block, mesh=mesh, in_specs=(row_spec, weight_spec, weight_spec, P(("data", "row"))), out_specs=row_spec, check_vma=NO)
```

```python
import functools

import jax
import jax.numpy as jnp
from jax import lax
from jax.experimental import pallas as pl
from jax.experimental.pallas import tpu as pltpu
from jax.sharding import PartitionSpec as P

HEAD_DIM = 128
CORES = 2
Q_TILE = 256
CHUNKS = 4
UNROLL = 2
LOG2E = 1.4426950408889634
BOTH = (0, 1)
YES, NO = True, False


MESH = pl.DeviceIdType.MESH


def near_x(x):
    return x + 1 - 2 * (x % 2)


def qkv_kernel(n_x, n_y, tok_ref, w_ref, wo_ref, seg_ref, q_ref, kv_ref, segs_ref, got_ref, xg, wg, acc, w_send, w_recv, d_send, d_recv, t_send, t_recv, y_send, y_recv, k_send, k_recv, l_sem, s_send, s_recv, o_send, o_recv):
    r, y = lax.axis_index("row"), lax.axis_index("col")
    x, c = r // CORES, r % CORES
    xn, xf = near_x(x), n_x - 1 - x
    xnf = n_x - 1 - xn
    half = x // (n_x // 2)
    before, after, across = (y + n_y - 1) % n_y, (y + 1) % n_y, (y + 2) % n_y
    rows, width = tok_ref.shape
    depth = w_ref.shape[0]
    part = w_ref.shape[1] // 2
    ctx = part - 2 * HEAD_DIM
    mid, cut, quarter = rows // 2, depth // 2, rows // 4
    near, far, core = {"row": CORES * xn + c}, {"row": CORES * xf + c}, {"row": CORES * x + 1 - c}
    up, down = {"col": after}, {"col": before}

    barrier = pltpu.get_barrier_semaphore()
    n_row = CORES * n_x
    row_peers = [{"row": (r + d) % n_row} for d in range(1, n_row)]
    for peer in row_peers + [up, down]:
        pl.semaphore_signal(barrier, inc=1, device_id=peer, device_id_type=MESH)
    pl.semaphore_wait(barrier, n_row + 1)

    started = []

    def send(src, dst, s_sem, r_sem, peer):
        copy = pltpu.make_async_remote_copy(src_ref=src, dst_ref=dst, send_sem=s_sem, recv_sem=r_sem, device_id=peer, device_id_type=MESH)
        copy.start()
        started.append(copy)
        return copy

    mine = pl.ds(pl.multiple_of(half * part, 128), part)
    theirs = pl.ds(pl.multiple_of((1 - half) * part, 128), part)

    def w_slot(chip, plane, i):
        return wg.at[chip, pl.ds(pl.multiple_of(plane * depth + i * cut, cut), cut), :]

    def send_w(kind, i):
        src_rows = pl.ds(i * cut, cut)
        if kind == 0:
            return send(w_ref.at[src_rows, mine], w_slot(x, c, i), w_send.at[0, i], w_recv.at[0, i], near)
        if kind == 1:
            return send(w_ref.at[src_rows, theirs], w_slot(x, c, i), w_send.at[1, i], w_recv.at[1, i], far)
        return send(w_slot(xf, c, i), w_slot(xf, c, i), w_send.at[2, i], w_recv.at[2, i], near)

    def share(chip, i, at):
        src = w_ref.at[pl.ds(i * cut, cut), mine] if at == 0 else w_slot(chip, c, i)
        return send(src, w_slot(chip, c, i), d_send.at[at, i], d_recv.at[at, i], core)

    def x_slot(b, at, lo, n):
        return xg.at[b, at, pl.ds(lo, n), :]

    def send_t(a):
        return send(tok_ref.at[pl.ds(a * mid, mid), :], x_slot(1, y, a * mid, mid), t_send.at[a], t_recv.at[a], far)

    def send_y(b, a, way):
        src = tok_ref.at[pl.ds(a * mid, mid), :] if b == 0 else x_slot(1, y, a * mid, mid)
        return send(src, x_slot(b, y, a * mid, mid), y_send.at[b, a, way], y_recv.at[b, a, way], (up, down)[way])

    def pass_y(b, a, way):
        at = (before, after)[way]
        piece = x_slot(b, at, a * mid + way * quarter, quarter)
        return send(piece, piece, y_send.at[b, a, 2 + way], y_recv.at[b, a, 2 + way], (up, down)[way])

    segs = [send(seg_ref, segs_ref.at[r], s_send.at[d], s_recv.at[d], peer) for d, peer in enumerate(row_peers)]
    w_far = [send_w(1, 0)]
    y_own = [[send_y(0, a, way) for way in BOTH] for a in BOTH]
    w_near = [send_w(0, 0)]
    tok = [send_t(0)]
    w_near.append(send_w(0, 1))
    w_far.append(send_w(1, 1))
    tok.append(send_t(1))
    chunk = depth // CHUNKS
    wo_got = [send(wo_ref.at[pl.ds(i * chunk, chunk), :], got_ref.at[1 + i], o_send.at[1 + i], o_recv.at[1 + i], far) for i in BOTH]
    locals_ = [
        pltpu.make_async_copy(seg_ref, segs_ref.at[r], l_sem.at[2]),
        pltpu.make_async_copy(tok_ref, xg.at[0, y], l_sem.at[0]),
        pltpu.make_async_copy(w_ref.at[:, mine], wg.at[x, pl.ds(pl.multiple_of(c * depth, depth), depth), :], l_sem.at[1]),
    ]
    for copy in locals_:
        copy.start()
    d_own = [share(x, i, 0) for i in BOTH]

    def multiply(b, lo, n, chip, first, last):
        tile = 2 * HEAD_DIM

        @pl.loop(0, part // tile)
        def _(j):
            cols = pl.ds(pl.multiple_of(j * tile, tile), tile)
            dot = jnp.dot(xg[b, chip, pl.ds(lo, n), :], wg[chip, :, cols], preferred_element_type=jnp.float32)
            if not first:
                dot = dot + acc[pl.ds(lo, n), cols]
            if not last:
                acc[pl.ds(lo, n), cols] = dot
            else:
                out = dot.astype(jnp.bfloat16)

                @pl.when(j < ctx // tile)
                def _():
                    q_ref[pl.ds(b * rows + lo, n), cols] = out

                @pl.when(j == ctx // tile)
                def _():
                    kv_ref[pl.ds(b * rows + lo, n), :] = out

    def kv_slot(s):
        return kv_ref.at[pl.ds(s * rows, rows), :]

    def kv_near(b):
        return send(kv_slot(b), kv_slot(2 + b), k_send.at[b], k_recv.at[b], near)

    def kv_core(s):
        return send(kv_slot(s), kv_slot(4 + s), k_send.at[2 + s], k_recv.at[2 + s], core)

    def relay(b, a):
        got = []
        for way in BOTH:
            (y_own if b == 0 else y_par)[a][way].wait_recv()
            got.append(pass_y(b, a, way))
        return got

    y_far = [relay(0, 0)]
    w_far[0].wait_recv()
    w_nf = [send_w(2, 0)]
    d_far = [share(xf, 0, 2)]
    w_near[0].wait_recv()
    d_near = [share(xn, 0, 1)]
    y_far.append(relay(0, 1))
    tok[0].wait_recv()
    y_par = [[send_y(1, 0, way) for way in BOTH]]
    w_near[1].wait_recv()
    d_near.append(share(xn, 1, 1))
    for pair in y_far:
        for copy in pair:
            copy.wait_recv()
    for copy in locals_:
        copy.wait()
    for copy in d_own:
        copy.wait_recv()
    multiply(0, 0, rows, x, YES, NO)
    for copy in d_near:
        copy.wait_recv()
    w_far[1].wait_recv()
    w_nf.append(send_w(2, 1))
    wo_got.append(send(wo_ref.at[pl.ds(0, chunk), :], got_ref.at[0], o_send.at[0], o_recv.at[0], near))
    d_far.append(share(xf, 1, 2))
    multiply(0, 0, rows, xn, NO, NO)
    w_nf[0].wait_recv()
    d_nf = [share(xnf, 0, 3)]
    y_pfar = [relay(1, 0)]
    tok[1].wait_recv()
    y_par.append([send_y(1, 1, way) for way in BOTH])
    for copy in d_far:
        copy.wait_recv()
    multiply(0, 0, rows, xf, NO, NO)
    w_nf[1].wait_recv()
    d_nf.append(share(xnf, 1, 3))
    for copy in d_nf:
        copy.wait_recv()
    multiply(0, 0, rows, xnf, NO, YES)
    for copy in y_pfar[0]:
        copy.wait_recv()
    multiply(1, 0, mid, y, YES, NO)
    k_near, k_core = [kv_near(0)], [kv_core(0)]
    multiply(1, 0, mid, before, NO, NO)
    y_pfar.append(relay(1, 1))
    multiply(1, 0, mid, after, NO, NO)
    multiply(1, 0, mid, across, NO, YES)
    multiply(1, mid, mid, y, YES, NO)
    multiply(1, mid, mid, before, NO, NO)
    multiply(1, mid, mid, after, NO, NO)
    k_near[0].wait_recv()
    k_core.append(kv_core(2))
    for copy in y_pfar[1]:
        copy.wait_recv()
    multiply(1, mid, mid, across, NO, YES)
    k_near.append(kv_near(1))
    k_core.append(kv_core(1))
    k_near[1].wait_recv()
    k_core.append(kv_core(3))
    for copy in k_core + wo_got + segs:
        copy.wait_recv()
    for copy in started:
        copy.wait_send()


def project_qkv(tokens, w_qkv, w_out, doc_ids, n_x, n_y):
    rows, width = tokens.shape
    depth, cols = w_qkv.shape
    part = cols // 2
    ctx = part - 2 * HEAD_DIM
    n_row = CORES * n_x
    dma = pltpu.SemaphoreType.DMA
    anywhere, vmem = pl.BlockSpec(memory_space=pl.ANY), pl.BlockSpec(memory_space=pltpu.VMEM)
    segs = doc_ids.reshape(rows // 128, 128)
    return pl.pallas_call(
        functools.partial(qkv_kernel, n_x, n_y),
        out_shape=(
            jax.ShapeDtypeStruct((2 * rows, ctx), jnp.bfloat16),
            jax.ShapeDtypeStruct((n_row * rows, 2 * HEAD_DIM), jnp.bfloat16),
            jax.ShapeDtypeStruct((n_row,) + segs.shape, jnp.int32),
            jax.ShapeDtypeStruct((3, depth // CHUNKS, w_out.shape[1]), jnp.bfloat16),
        ),
        in_specs=[anywhere] * 4,
        out_specs=(vmem, vmem, vmem, anywhere),
        scratch_shapes=[
            pltpu.VMEM((2, n_y, rows, width), jnp.bfloat16),
            pltpu.VMEM((n_x, CORES * depth, part), jnp.bfloat16),
            pltpu.VMEM((rows, part), jnp.float32),
            dma((3, 2)), dma((3, 2)), dma((4, 2)), dma((4, 2)), dma((2,)), dma((2,)),
            dma((2, 2, 4)), dma((2, 2, 4)), dma((6,)), dma((6,)), dma((3,)),
            dma((n_row - 1,)), dma((n_row - 1,)), dma((3,)), dma((3,)),
        ],
        compiler_params=pltpu.CompilerParams(collective_id=0, has_side_effects=YES, vmem_limit_bytes=60 * 1024 * 1024),
        cost_estimate=pl.CostEstimate(flops=4 * rows * n_y * width * part, bytes_accessed=2 * depth * cols, transcendentals=0),
        name="project_qkv",
    )(tokens, w_qkv, w_out, segs)


def attend_kernel(n_x, n_y, q_ref, kv_ref, segs_ref, got_ref, w_ref, out_ref, wo, panel, obuf, sbuf, segq, mbuf, lbuf, abuf, n_send, n_recv, f_send, f_recv, d_send, d_recv, t_send, t_recv, y_send, y_recv, l_sem):
    r, y = lax.axis_index("row"), lax.axis_index("col")
    x, c = r // CORES, r % CORES
    xn, xf = near_x(x), n_x - 1 - x
    xnf = n_x - 1 - xn
    half = x // (n_x // 2)
    before, after, across = (y + n_y - 1) % n_y, (y + 1) % n_y, (y + 2) % n_y
    rows = out_ref.shape[0]
    keys = kv_ref.shape[0]
    chunk = w_ref.shape[0] // CHUNKS
    width = w_ref.shape[1]
    heads = q_ref.shape[1] // HEAD_DIM
    tiles = 2 * rows // Q_TILE
    units = tiles * heads
    eighth = Q_TILE // 2
    coef = HEAD_DIM ** -0.5 * LOG2E
    lowest = jnp.finfo(jnp.float32).min
    near, far, core = {"row": CORES * xn + c}, {"row": CORES * xf + c}, {"row": CORES * x + 1 - c}
    up, down = {"col": after}, {"col": before}

    barrier = pltpu.get_barrier_semaphore()
    for peer in (near, far, core, up, down):
        pl.semaphore_signal(barrier, inc=1, device_id=peer, device_id_type=MESH)
    pl.semaphore_wait(barrier, 5)

    started = []

    def send(src, dst, s_sem, r_sem, peer):
        copy = pltpu.make_async_remote_copy(src_ref=src, dst_ref=dst, send_sem=s_sem, recv_sem=r_sem, device_id=peer, device_id_type=MESH)
        copy.start()
        started.append(copy)
        return copy

    def w_slot(k, chip):
        return wo.at[k, pl.ds(pl.multiple_of((CORES * chip + c) * chunk, chunk), chunk), :]

    def w_mine(k):
        return w_ref.at[pl.ds(k * chunk, chunk), :]

    def share(k, origin, src=None):
        slot = w_slot(k, (x, xn, xf, xnf)[origin])
        return send(slot if src is None else src, slot, d_send.at[k, origin], d_recv.at[k, origin], core)

    def to_near(k, src, chip):
        return send(src, w_slot(k, chip), n_send.at[k, 0], n_recv.at[k, 0], near)

    def to_far(k, src, chip):
        return send(src, w_slot(k, chip), f_send.at[k, 0], f_recv.at[k, 0], far)

    direct = {2: to_near(2, w_mine(2), x), 3: to_near(3, w_mine(3), x)}
    straight = {2: to_far(2, w_mine(2), x), 3: to_far(3, w_mine(3), x)}
    direct[1] = to_near(1, w_mine(1), x)
    corner = {0: send(got_ref.at[1], w_slot(0, xf), n_send.at[0, 1], n_recv.at[0, 1], near)}
    corner[1] = send(got_ref.at[2], w_slot(1, xf), n_send.at[1, 1], n_recv.at[1, 1], near)
    places = [(w_mine(k), w_slot(k, x)) for k in range(CHUNKS)]
    places += [(got_ref.at[0], w_slot(0, xn)), (got_ref.at[1], w_slot(0, xf)), (got_ref.at[2], w_slot(1, xf))]
    placed = [pltpu.make_async_copy(src, dst, l_sem.at[i]) for i, (src, dst) in enumerate(places)]
    for copy in placed:
        copy.start()
    shared = [share(k, 0, w_mine(k)) for k in range(CHUNKS)]
    shared += [share(0, 1, got_ref.at[0]), share(0, 2, got_ref.at[1]), share(1, 2, got_ref.at[2])]

    for i in range(2 * rows // 128):
        at = r if i < rows // 128 else CORES * xf + c
        line = segs_ref[at, pl.ds(i % (rows // 128), 1), :].astype(jnp.float32)
        segq[pl.ds(i * 128, 128), :] = jnp.broadcast_to(line, (128, 128)).T

    def key_row(j):
        odd, fam, plane = j % 2, (j // 2) % 2, j // 4
        base = x + fam * (xn - x)
        chip = base + odd * (n_x - 1 - 2 * base)
        return CORES * chip + c + plane * (1 - 2 * c)

    blocks = keys // rows
    lanes = rows // 128

    def scores(u, j):
        b, tile, h = u % 3, (u // heads + tiles // 2) % tiles, u % heads
        q = q_ref[pl.ds(pl.multiple_of(tile * Q_TILE, Q_TILE), Q_TILE), pl.ds(pl.multiple_of(h * HEAD_DIM, HEAD_DIM), HEAD_DIM)]
        k = kv_ref[pl.ds(pl.multiple_of(j * rows, rows), rows), pl.ds(0, HEAD_DIM)]
        s = lax.dot_general(q, k, (((1,), (1,)), ((), ())), preferred_element_type=jnp.float32)
        own = segq[pl.ds(pl.multiple_of(tile * Q_TILE, Q_TILE), Q_TILE), :]
        seg = segs_ref[key_row(j)].astype(jnp.float32)
        top = mbuf[b]
        for i in range(lanes):
            part = jnp.where(own == seg[i:i + 1, :], s[:, i * 128:(i + 1) * 128], lowest)
            sbuf[b, j * lanes + i] = part
            top = jnp.maximum(top, part)
        mbuf[b] = top

    def powers(u, j):
        b = u % 3
        top = mbuf[b]
        total = lbuf[b]
        for i in range(lanes):
            e = jnp.exp2((sbuf[b, j * lanes + i] - top) * coef)
            sbuf[b, j * lanes + i] = e
            total = total + e
        lbuf[b] = total

    def context(u, j):
        b = u % 3
        inv = lbuf[b]
        p = jnp.concatenate([(sbuf[b, j * lanes + i] * inv).astype(jnp.bfloat16) for i in range(lanes)], axis=1)
        v = kv_ref[pl.ds(pl.multiple_of(j * rows, rows), rows), pl.ds(HEAD_DIM, HEAD_DIM)]
        abuf[...] += jnp.dot(p, v, preferred_element_type=jnp.float32)

    def open_unit(u, a, b, e):
        if a:
            mbuf[u % 3] = jnp.full(mbuf.shape[1:], lowest, jnp.float32)
        if b:
            lbuf[(u - 1) % 3] = jnp.zeros(lbuf.shape[1:], jnp.float32)
        if e:
            abuf[...] = jnp.zeros(abuf.shape, jnp.float32)

    def close_unit(u, a, b, e):
        if a:
            mbuf[u % 3] = jnp.broadcast_to(jnp.max(mbuf[u % 3], axis=1, keepdims=YES), mbuf.shape[1:])
        if b:
            lbuf[(u - 1) % 3] = 1.0 / jnp.broadcast_to(jnp.sum(lbuf[(u - 1) % 3], axis=1, keepdims=YES), lbuf.shape[1:])
        if e:
            tile, h = (u - 2) // heads, (u - 2) % heads
            out = abuf[...].astype(jnp.bfloat16)
            per = heads // CHUNKS
            lo = pl.multiple_of((h % per) * HEAD_DIM, HEAD_DIM)
            mine = pl.multiple_of((CORES * y + half) * chunk, chunk)

            at = pl.ds(pl.multiple_of(tile % (tiles // 2) * Q_TILE, Q_TILE), Q_TILE)

            @pl.when(tile >= tiles // 2)
            def _():
                panel[h // per, at, pl.ds(pl.multiple_of(mine + lo, HEAD_DIM), HEAD_DIM)] = out

            @pl.when(tile < tiles // 2)
            def _():
                obuf[h // per, at, pl.ds(lo, HEAD_DIM)] = out

    def unit(u, a, b, e):
        open_unit(u, a, b, e)

        @pl.loop(0, blocks // UNROLL)
        def _(jj):
            for i in range(UNROLL):
                j = jj * UNROLL + i
                if a:
                    scores(u, j)
                if b:
                    powers(u - 1, j)
                if e:
                    context(u - 2, j)

        close_unit(u, a, b, e)

    group = CHUNKS // 2

    def o_slot(yy, f, g, lo, n):
        hh = half + f * (1 - 2 * half)
        return panel.at[pl.ds(g * group, group), pl.ds(lo, n), pl.ds(pl.multiple_of((CORES * yy + hh) * chunk, chunk), chunk)]

    def send_o(a, g):
        return pltpu.make_async_remote_copy(
            src_ref=obuf.at[pl.ds(g * group, group), pl.ds(a * Q_TILE, Q_TILE), :], dst_ref=o_slot(y, 0, g, a * Q_TILE, Q_TILE),
            send_sem=t_send.at[a, g], recv_sem=t_recv.at[a, g], device_id=far, device_id_type=MESH)

    def y_copy(f, a, g, way):
        piece = o_slot(y, f, g, a * Q_TILE, Q_TILE)
        return pltpu.make_async_remote_copy(src_ref=piece, dst_ref=piece, send_sem=y_send.at[f, a, g, way], recv_sem=y_recv.at[f, a, g, way], device_id=(up, down)[way], device_id_type=MESH)

    def y_pass(f, a, g, way):
        piece = o_slot((before, after)[way], f, g, a * Q_TILE + way * eighth, eighth)
        return pltpu.make_async_remote_copy(src_ref=piece, dst_ref=piece, send_sem=y_send.at[f, a, g, 2 + way], recv_sem=y_recv.at[f, a, g, 2 + way], device_id=(up, down)[way], device_id_type=MESH)

    def w_copy(kind, k):
        if kind == 0:
            return pltpu.make_async_remote_copy(src_ref=w_slot(k, xn), dst_ref=w_slot(k, xn), send_sem=f_send.at[k, 1], recv_sem=f_recv.at[k, 1], device_id=far, device_id_type=MESH)
        slot = w_slot(k, (x, xn, xf, xnf)[kind])
        return pltpu.make_async_remote_copy(src_ref=slot, dst_ref=slot, send_sem=d_send.at[k, kind], recv_sem=d_recv.at[k, kind], device_id=core, device_id_type=MESH)

    def near_in(k):
        direct[k].wait_recv()
        if k >= 2:
            w_copy(0, k).start()
        w_copy(1, k).start()

    def far_in(k):
        straight[k].wait_recv()
        w_copy(2, k).start()

    def corner_in(k):
        (corner[k] if k < 2 else w_copy(0, k)).wait_recv()
        w_copy(3, k).start()

    def y_start(f, a, g):
        for way in BOTH:
            y_copy(f, a, g, way).start()

    def y_relay(f, a, g):
        for way in BOTH:
            y_copy(f, a, g, way).wait_recv()
            y_pass(f, a, g, way).start()

    def o_in(a, g):
        send_o(a, g).wait_recv()
        y_start(1, a, g)

    def o_out(a, g):
        send_o(a, g).start()

    events = (
        (7, o_out, 0, 0), (11, o_out, 0, 1), (12, near_in, 2), (12, far_in, 2),
        (15, o_out, 1, 0), (19, o_out, 1, 1), (19, o_in, 0, 0), (20, near_in, 3), (20, far_in, 3), (21, o_in, 0, 1),
        (22, y_relay, 1, 0, 0), (23, y_start, 0, 0, 0), (24, y_relay, 1, 0, 1), (25, near_in, 1),
        (26, y_relay, 0, 0, 0), (27, y_start, 0, 0, 1), (29, corner_in, 2), (30, y_relay, 0, 0, 1),
        (30, o_in, 1, 0), (31, y_start, 0, 1, 0),
    )

    unit(0, YES, NO, NO)
    unit(1, YES, YES, NO)

    @pl.loop(2, units)
    def _(u):
        for at in sorted({event[0] for event in events}):
            @pl.when(u == at)
            def _(at=at):
                for when, step, *which in events:
                    if when == at:
                        step(*which)
        unit(u, YES, YES, YES)

    unit(units, NO, YES, YES)
    unit(units + 1, NO, NO, YES)

    def multiply(a, k, first, last):
        tile = 2 * HEAD_DIM

        @pl.loop(0, width // tile)
        def _(n):
            cols = pl.ds(pl.multiple_of(n * tile, tile), tile)
            dot = jnp.dot(panel[k, pl.ds(a * Q_TILE, Q_TILE), :], wo[k, :, cols], preferred_element_type=jnp.float32)
            per = tile // 128
            if not first:
                dot = dot + jnp.concatenate([sbuf[a, n * per + i] for i in range(per)], axis=1)
            if not last:
                for i in range(per):
                    sbuf[a, n * per + i] = dot[:, i * 128:(i + 1) * 128]
            else:
                out_ref[pl.ds(a * Q_TILE, Q_TILE), cols] = dot.astype(jnp.bfloat16)

    def shares_in(k, kinds):
        for kind in kinds:
            w_copy(kind, k).wait_recv()

    def rows_in(a, g):
        for f in BOTH:
            for way in BOTH:
                y_pass(f, a, g, way).wait_recv()

    passed = (1, 2, 3)
    o_in(1, 1)
    y_start(0, 1, 1)
    y_relay(1, 1, 0)
    y_relay(0, 1, 0)
    corner_in(0)
    for copy in placed:
        copy.wait()
    for copy in shared:
        copy.wait_recv()
    rows_in(0, 0)
    rows_in(0, 1)
    shares_in(2, passed)
    multiply(0, 2, YES, NO)
    y_relay(1, 1, 1)
    y_relay(0, 1, 1)
    shares_in(0, passed[2:])
    multiply(0, 0, NO, NO)
    rows_in(1, 0)
    multiply(1, 0, YES, NO)
    rows_in(1, 1)
    multiply(1, 2, NO, NO)
    corner_in(3)
    corner_in(1)
    shares_in(3, passed)
    for a in BOTH:
        multiply(a, 3, NO, NO)
    shares_in(1, passed[::2])
    for a in BOTH:
        multiply(a, 1, NO, YES)
    for copy in started:
        copy.wait_send()
    for k in (2, 3):
        w_copy(0, k).wait_send()
        for kind in (1, 2, 3):
            w_copy(kind, k).wait_send()
    for kind, k in ((3, 0), (1, 1), (3, 1)):
        w_copy(kind, k).wait_send()
    for a in BOTH:
        for g in BOTH:
            send_o(a, g).wait_send()
            for f in BOTH:
                for way in BOTH:
                    y_copy(f, a, g, way).wait_send()
                    y_pass(f, a, g, way).wait_send()


def attend_project(q, kv, segs, got, w_out, n_x, n_y):
    rows, ctx = q.shape[0] // 2, q.shape[1]
    keys = kv.shape[0]
    depth, width = w_out.shape
    n_row = CORES * n_x
    chunk = depth // CHUNKS
    dma = pltpu.SemaphoreType.DMA
    anywhere, vmem = pl.BlockSpec(memory_space=pl.ANY), pl.BlockSpec(memory_space=pltpu.VMEM)
    return pl.pallas_call(
        functools.partial(attend_kernel, n_x, n_y),
        out_shape=jax.ShapeDtypeStruct((rows, width), jnp.bfloat16),
        in_specs=[vmem, vmem, vmem, anywhere, anywhere],
        out_specs=vmem,
        scratch_shapes=[
            pltpu.VMEM((CHUNKS, n_row * chunk, width), jnp.bfloat16),
            pltpu.VMEM((CHUNKS, rows, n_row * chunk), jnp.bfloat16),
            pltpu.VMEM((CHUNKS, rows, chunk), jnp.bfloat16),
            pltpu.VMEM((3, keys // 128, Q_TILE, 128), jnp.float32),
            pltpu.VMEM((2 * rows, 128), jnp.float32),
            pltpu.VMEM((3, Q_TILE, 128), jnp.float32),
            pltpu.VMEM((3, Q_TILE, 128), jnp.float32),
            pltpu.VMEM((Q_TILE, HEAD_DIM), jnp.float32),
            dma((CHUNKS, 2)), dma((CHUNKS, 2)), dma((CHUNKS, 2)), dma((CHUNKS, 2)),
            dma((CHUNKS, 4)), dma((CHUNKS, 4)), dma((2, 2)), dma((2, 2)),
            dma((2, 2, 2, 4)), dma((2, 2, 2, 4)), dma((CHUNKS + 3,)),
        ],
        compiler_params=pltpu.CompilerParams(collective_id=1, has_side_effects=YES, vmem_limit_bytes=63 * 1024 * 1024),
        cost_estimate=pl.CostEstimate(flops=8 * rows * ctx * keys, bytes_accessed=4 * depth * width, transcendentals=0),
        name="attend_project",
    )(q, kv, segs, got, w_out)


def solution(mesh):
    n_x, n_y = mesh.shape["row"] // CORES, mesh.shape["col"]

    def local_block(tokens, w_qkv, w_out, doc_ids):
        q, kv, segs, got = project_qkv(tokens, w_qkv, w_out, doc_ids, n_x, n_y)
        return attend_project(q, kv, segs, got, w_out, n_x, n_y)

    row_spec = P(("data", "row"), "col")
    weight_spec = P("row", "col")
    return jax.shard_map(local_block, mesh=mesh, in_specs=(row_spec, weight_spec, weight_spec, P(("data", "row"))), out_specs=row_spec, check_vma=NO)
```

```python
import functools

import jax
import jax.numpy as jnp
from jax import lax
from jax.experimental import pallas as pl
from jax.experimental.pallas import tpu as pltpu
from jax.sharding import PartitionSpec as P

HEAD_DIM = 128
CORES = 2
Q_TILE = 256
CHUNKS = 4
UNROLL = 2
LOG2E = 1.4426950408889634
BOTH = (0, 1)
YES, NO = True, False


MESH = pl.DeviceIdType.MESH


def near_x(x):
    return x + 1 - 2 * (x % 2)


def qkv_kernel(n_x, n_y, tok_ref, w_ref, wo_ref, seg_ref, q_ref, kv_ref, segs_ref, got_ref, xg, wg, acc, w_send, w_recv, d_send, d_recv, t_send, t_recv, y_send, y_recv, k_send, k_recv, s_send, s_recv, o_send, o_recv, l_sem):
    r, y = lax.axis_index("row"), lax.axis_index("col")
    x, c = r // CORES, r % CORES
    xn, xf = near_x(x), n_x - 1 - x
    xnf = n_x - 1 - xn
    half = x // (n_x // 2)
    before, after, across = (y + n_y - 1) % n_y, (y + 1) % n_y, (y + 2) % n_y
    rows, width = tok_ref.shape
    depth = w_ref.shape[0]
    part = w_ref.shape[1] // 2
    ctx = part - 2 * HEAD_DIM
    mid, cut, quarter = rows // 2, depth // 2, rows // 4
    near, far, core = {"row": CORES * xn + c}, {"row": CORES * xf + c}, {"row": CORES * x + 1 - c}
    up, down = {"col": after}, {"col": before}

    barrier = pltpu.get_barrier_semaphore()
    n_row = CORES * n_x
    row_peers = [{"row": (r + d) % n_row} for d in range(1, n_row)]
    for peer in row_peers + [up, down]:
        pl.semaphore_signal(barrier, inc=1, device_id=peer, device_id_type=MESH)
    pl.semaphore_wait(barrier, n_row + 1)

    started = []

    def send(src, dst, s_sem, r_sem, peer):
        copy = pltpu.make_async_remote_copy(src_ref=src, dst_ref=dst, send_sem=s_sem, recv_sem=r_sem, device_id=peer, device_id_type=MESH)
        copy.start()
        started.append(copy)
        return copy

    mine = pl.ds(pl.multiple_of(half * part, 128), part)
    theirs = pl.ds(pl.multiple_of((1 - half) * part, 128), part)

    def w_slot(chip, plane, i):
        return wg.at[chip, pl.ds(pl.multiple_of(plane * depth + i * cut, cut), cut), :]

    def send_w(kind, i):
        src_rows = pl.ds(i * cut, cut)
        if kind == 0:
            return send(w_ref.at[src_rows, mine], w_slot(x, c, i), w_send.at[0, i], w_recv.at[0, i], near)
        if kind == 1:
            return send(w_ref.at[src_rows, theirs], w_slot(x, c, i), w_send.at[1, i], w_recv.at[1, i], far)
        return send(w_slot(xf, c, i), w_slot(xf, c, i), w_send.at[2, i], w_recv.at[2, i], near)

    def share(chip, i, at):
        src = w_ref.at[pl.ds(i * cut, cut), mine] if at == 0 else w_slot(chip, c, i)
        return send(src, w_slot(chip, c, i), d_send.at[at, i], d_recv.at[at, i], core)

    def x_slot(b, at, lo, n):
        return xg.at[b, at, pl.ds(lo, n), :]

    def send_t(a):
        return send(tok_ref.at[pl.ds(a * mid, mid), :], x_slot(1, y, a * mid, mid), t_send.at[a], t_recv.at[a], far)

    def send_y(b, a, way):
        src = tok_ref.at[pl.ds(a * mid, mid), :] if b == 0 else x_slot(1, y, a * mid, mid)
        return send(src, x_slot(b, y, a * mid, mid), y_send.at[b, a, way], y_recv.at[b, a, way], (up, down)[way])

    def pass_y(b, a, way):
        at = (before, after)[way]
        piece = x_slot(b, at, a * mid + way * quarter, quarter)
        return send(piece, piece, y_send.at[b, a, 2 + way], y_recv.at[b, a, 2 + way], (up, down)[way])

    segs = [send(seg_ref, segs_ref.at[r], s_send.at[d], s_recv.at[d], peer) for d, peer in enumerate(row_peers)]
    w_far = [send_w(1, 0)]
    y_own = [[send_y(0, a, way) for way in BOTH] for a in BOTH]
    w_near = [send_w(0, 0)]
    tok = [send_t(0)]
    w_near.append(send_w(0, 1))
    w_far.append(send_w(1, 1))
    tok.append(send_t(1))
    chunk = depth // CHUNKS
    wo_got = [send(wo_ref.at[pl.ds(i * chunk, chunk), :], got_ref.at[1 + i], o_send.at[1 + i], o_recv.at[1 + i], far) for i in BOTH]
    locals_ = [
        pltpu.make_async_copy(seg_ref, segs_ref.at[r], l_sem.at[2]),
        pltpu.make_async_copy(tok_ref, xg.at[0, y], l_sem.at[0]),
        pltpu.make_async_copy(w_ref.at[:, mine], wg.at[x, pl.ds(pl.multiple_of(c * depth, depth), depth), :], l_sem.at[1]),
    ]
    for copy in locals_:
        copy.start()
    d_own = [share(x, i, 0) for i in BOTH]

    def multiply(b, lo, n, chip, first, last):
        tile = 2 * HEAD_DIM

        @pl.loop(0, part // tile)
        def _(j):
            cols = pl.ds(pl.multiple_of(j * tile, tile), tile)
            dot = jnp.dot(xg[b, chip, pl.ds(lo, n), :], wg[chip, :, cols], preferred_element_type=jnp.float32)
            if not first:
                dot = dot + acc[pl.ds(lo, n), cols]
            if not last:
                acc[pl.ds(lo, n), cols] = dot
            else:
                out = dot.astype(jnp.bfloat16)

                @pl.when(j < ctx // tile)
                def _():
                    q_ref[pl.ds(b * rows + lo, n), cols] = out

                @pl.when(j == ctx // tile)
                def _():
                    kv_ref[pl.ds(b * rows + lo, n), :] = out

    def kv_slot(s):
        return kv_ref.at[pl.ds(s * rows, rows), :]

    def kv_near(b):
        return send(kv_slot(b), kv_slot(2 + b), k_send.at[b], k_recv.at[b], near)

    def kv_core(s):
        return send(kv_slot(s), kv_slot(4 + s), k_send.at[2 + s], k_recv.at[2 + s], core)

    def relay(b, a):
        got = []
        for way in BOTH:
            (y_own if b == 0 else y_par)[a][way].wait_recv()
            got.append(pass_y(b, a, way))
        return got

    y_far = [relay(0, 0)]
    w_far[0].wait_recv()
    w_nf = [send_w(2, 0)]
    d_far = [share(xf, 0, 2)]
    w_near[0].wait_recv()
    d_near = [share(xn, 0, 1)]
    y_far.append(relay(0, 1))
    tok[0].wait_recv()
    y_par = [[send_y(1, 0, way) for way in BOTH]]
    w_near[1].wait_recv()
    d_near.append(share(xn, 1, 1))
    for pair in y_far:
        for copy in pair:
            copy.wait_recv()
    for copy in locals_:
        copy.wait()
    for copy in d_own:
        copy.wait_recv()
    multiply(0, 0, rows, x, YES, NO)
    for copy in d_near:
        copy.wait_recv()
    w_far[1].wait_recv()
    w_nf.append(send_w(2, 1))
    wo_got.append(send(wo_ref.at[pl.ds(0, chunk), :], got_ref.at[0], o_send.at[0], o_recv.at[0], near))
    d_far.append(share(xf, 1, 2))
    multiply(0, 0, rows, xn, NO, NO)
    w_nf[0].wait_recv()
    d_nf = [share(xnf, 0, 3)]
    y_pfar = [relay(1, 0)]
    tok[1].wait_recv()
    y_par.append([send_y(1, 1, way) for way in BOTH])
    for copy in d_far:
        copy.wait_recv()
    multiply(0, 0, rows, xf, NO, NO)
    w_nf[1].wait_recv()
    d_nf.append(share(xnf, 1, 3))
    for copy in d_nf:
        copy.wait_recv()
    multiply(0, 0, rows, xnf, NO, YES)
    for copy in y_pfar[0]:
        copy.wait_recv()
    multiply(1, 0, mid, y, YES, NO)
    k_near, k_core = [kv_near(0)], [kv_core(0)]
    multiply(1, 0, mid, before, NO, NO)
    y_pfar.append(relay(1, 1))
    multiply(1, 0, mid, after, NO, NO)
    multiply(1, 0, mid, across, NO, YES)
    multiply(1, mid, mid, y, YES, NO)
    multiply(1, mid, mid, before, NO, NO)
    multiply(1, mid, mid, after, NO, NO)
    k_near[0].wait_recv()
    k_core.append(kv_core(2))
    for copy in y_pfar[1]:
        copy.wait_recv()
    multiply(1, mid, mid, across, NO, YES)
    k_near.append(kv_near(1))
    k_core.append(kv_core(1))
    k_near[1].wait_recv()
    k_core.append(kv_core(3))
    for copy in k_core + wo_got + segs:
        copy.wait_recv()
    for copy in started:
        copy.wait_send()


def project_qkv(tokens, w_qkv, w_out, doc_ids, n_x, n_y):
    rows, width = tokens.shape
    depth, cols = w_qkv.shape
    part = cols // 2
    ctx = part - 2 * HEAD_DIM
    n_row = CORES * n_x
    dma = pltpu.SemaphoreType.DMA
    anywhere, vmem = pl.BlockSpec(memory_space=pl.ANY), pl.BlockSpec(memory_space=pltpu.VMEM)
    segs = doc_ids.reshape(rows // 128, 128)
    return pl.pallas_call(
        functools.partial(qkv_kernel, n_x, n_y),
        out_shape=(
            jax.ShapeDtypeStruct((2 * rows, ctx), jnp.bfloat16),
            jax.ShapeDtypeStruct((n_row * rows, 2 * HEAD_DIM), jnp.bfloat16),
            jax.ShapeDtypeStruct((n_row,) + segs.shape, jnp.int32),
            jax.ShapeDtypeStruct((3, depth // CHUNKS, w_out.shape[1]), jnp.bfloat16),
        ),
        in_specs=[anywhere] * 4,
        out_specs=(vmem, vmem, vmem, anywhere),
        scratch_shapes=[
            pltpu.VMEM((2, n_y, rows, width), jnp.bfloat16),
            pltpu.VMEM((n_x, CORES * depth, part), jnp.bfloat16),
            pltpu.VMEM((rows, part), jnp.float32),
            *[dma(shape) for shape in ((3, 2), (4, 2), (2,), (2, 2, 4), (6,), (n_row - 1,), (3,)) for _ in BOTH],
            dma((3,)),
        ],
        compiler_params=pltpu.CompilerParams(collective_id=0, has_side_effects=YES, vmem_limit_bytes=60 * 1024 * 1024),
        cost_estimate=pl.CostEstimate(flops=4 * rows * n_y * width * part, bytes_accessed=2 * depth * cols, transcendentals=0),
        name="project_qkv",
    )(tokens, w_qkv, w_out, segs)


def attend_kernel(n_x, n_y, q_ref, kv_ref, segs_ref, got_ref, w_ref, out_ref, wo, panel, obuf, buf_a, buf_b, buf_c, segq, mbuf, lbuf, abuf, n_send, n_recv, f_send, f_recv, d_send, d_recv, t_send, t_recv, y_send, y_recv, l_sem):
    r, y = lax.axis_index("row"), lax.axis_index("col")
    x, c = r // CORES, r % CORES
    xn, xf = near_x(x), n_x - 1 - x
    xnf = n_x - 1 - xn
    half = x // (n_x // 2)
    before, after, across = (y + n_y - 1) % n_y, (y + 1) % n_y, (y + 2) % n_y
    rows = out_ref.shape[0]
    keys = kv_ref.shape[0]
    chunk = w_ref.shape[0] // CHUNKS
    width = w_ref.shape[1]
    heads = q_ref.shape[1] // HEAD_DIM
    tiles = 2 * rows // Q_TILE
    units = tiles * heads
    eighth = Q_TILE // 2
    coef = HEAD_DIM ** -0.5 * LOG2E
    lowest = jnp.finfo(jnp.float32).min
    near, far, core = {"row": CORES * xn + c}, {"row": CORES * xf + c}, {"row": CORES * x + 1 - c}
    up, down = {"col": after}, {"col": before}

    barrier = pltpu.get_barrier_semaphore()
    for peer in (near, far, core, up, down):
        pl.semaphore_signal(barrier, inc=1, device_id=peer, device_id_type=MESH)
    pl.semaphore_wait(barrier, 5)

    started = []

    def send(src, dst, s_sem, r_sem, peer):
        copy = pltpu.make_async_remote_copy(src_ref=src, dst_ref=dst, send_sem=s_sem, recv_sem=r_sem, device_id=peer, device_id_type=MESH)
        copy.start()
        started.append(copy)
        return copy

    def w_slot(k, chip):
        return wo.at[k, pl.ds(pl.multiple_of((CORES * chip + c) * chunk, chunk), chunk), :]

    def w_mine(k):
        return w_ref.at[pl.ds(k * chunk, chunk), :]

    def share(k, origin, src=None):
        slot = w_slot(k, (x, xn, xf, xnf)[origin])
        return send(slot if src is None else src, slot, d_send.at[k, origin], d_recv.at[k, origin], core)

    def remote(src, dst, s_sem, r_sem, peer):
        return pltpu.make_async_remote_copy(src_ref=src, dst_ref=dst, send_sem=s_sem, recv_sem=r_sem, device_id=peer, device_id_type=MESH)

    def to_near(k):
        return remote(w_mine(k), w_slot(k, x), n_send.at[k, 0], n_recv.at[k, 0], near)

    def to_far(k):
        return remote(w_mine(k), w_slot(k, x), f_send.at[k, 0], f_recv.at[k, 0], far)

    def corner(k):
        return remote(got_ref.at[1 + k], w_slot(k, xf), n_send.at[k, 1], n_recv.at[k, 1], near)

    def begin(copy, k):
        copy(k).start()

    begin(to_near, 2)
    begin(to_far, 2)
    places = [(w_mine(k), w_slot(k, x)) for k in range(CHUNKS)]
    places += [(got_ref.at[0], w_slot(0, xn)), (got_ref.at[1], w_slot(0, xf)), (got_ref.at[2], w_slot(1, xf))]
    placed = [pltpu.make_async_copy(src, dst, l_sem.at[i]) for i, (src, dst) in enumerate(places)]
    for copy in placed:
        copy.start()
    shared = [share(k, 0, w_mine(k)) for k in range(CHUNKS)]
    shared += [share(0, 1, got_ref.at[0]), share(0, 2, got_ref.at[1]), share(1, 2, got_ref.at[2])]

    for i in range(2 * rows // 128):
        at = r if i < rows // 128 else CORES * xf + c
        line = segs_ref[at, pl.ds(i % (rows // 128), 1), :].astype(jnp.float32)
        segq[pl.ds(i * 128, 128), :] = jnp.broadcast_to(line, (128, 128)).T

    def key_row(j):
        odd, fam, plane = j % 2, (j // 2) % 2, j // 4
        base = x + fam * (xn - x)
        chip = base + odd * (n_x - 1 - 2 * base)
        return CORES * chip + c + plane * (1 - 2 * c)

    blocks = keys // rows
    lanes = rows // 128
    bufs = (buf_a, buf_b, buf_c)
    n_buf = len(bufs)

    def scores(b, u, j):
        tile, h = (u // heads + tiles // 2) % tiles, u % heads
        q = q_ref[pl.ds(pl.multiple_of(tile * Q_TILE, Q_TILE), Q_TILE), pl.ds(pl.multiple_of(h * HEAD_DIM, HEAD_DIM), HEAD_DIM)]
        k = kv_ref[pl.ds(pl.multiple_of(j * rows, rows), rows), pl.ds(0, HEAD_DIM)]
        s = lax.dot_general(q, k, (((1,), (1,)), ((), ())), preferred_element_type=jnp.float32)
        own = segq[pl.ds(pl.multiple_of(tile * Q_TILE, Q_TILE), Q_TILE), :]
        seg = segs_ref[key_row(j)].astype(jnp.float32)
        top = mbuf[b]
        for i in range(lanes):
            part = jnp.where(own == seg[i:i + 1, :], s[:, i * 128:(i + 1) * 128], lowest)
            bufs[b][j * lanes + i] = part
            top = jnp.maximum(top, part)
        mbuf[b] = top

    def powers(b, j):
        top = mbuf[b]
        total = lbuf[b]
        for i in range(lanes):
            e = jnp.exp2((bufs[b][j * lanes + i] - top) * coef)
            bufs[b][j * lanes + i] = e
            total = total + e
        lbuf[b] = total

    def context(b, j):
        inv = lbuf[b]
        p = jnp.concatenate([(bufs[b][j * lanes + i] * inv).astype(jnp.bfloat16) for i in range(lanes)], axis=1)
        v = kv_ref[pl.ds(pl.multiple_of(j * rows, rows), rows), pl.ds(HEAD_DIM, HEAD_DIM)]
        abuf[...] += jnp.dot(p, v, preferred_element_type=jnp.float32)

    def open_unit(s, a, b, e):
        if a:
            mbuf[s] = jnp.full(mbuf.shape[1:], lowest, jnp.float32)
        if b:
            lbuf[(s - 1) % n_buf] = jnp.zeros(lbuf.shape[1:], jnp.float32)
        if e:
            abuf[...] = jnp.zeros(abuf.shape, jnp.float32)

    def close_unit(s, u, a, b, e):
        if a:
            mbuf[s] = jnp.broadcast_to(jnp.max(mbuf[s], axis=1, keepdims=YES), mbuf.shape[1:])
        if b:
            lbuf[(s - 1) % n_buf] = 1.0 / jnp.broadcast_to(jnp.sum(lbuf[(s - 1) % n_buf], axis=1, keepdims=YES), lbuf.shape[1:])
        if e:
            tile, h = (u - 2) // heads, (u - 2) % heads
            out = abuf[...].astype(jnp.bfloat16)
            per = heads // CHUNKS
            lo = pl.multiple_of((h % per) * HEAD_DIM, HEAD_DIM)
            mine = pl.multiple_of((CORES * y + half) * chunk, chunk)

            at = pl.ds(pl.multiple_of(tile % (tiles // 2) * Q_TILE, Q_TILE), Q_TILE)

            @pl.when(tile >= tiles // 2)
            def _():
                panel[h // per, at, pl.ds(pl.multiple_of(mine + lo, HEAD_DIM), HEAD_DIM)] = out

            @pl.when(tile < tiles // 2)
            def _():
                obuf[h // per, at, pl.ds(lo, HEAD_DIM)] = out

    def unit(s, u, a, b, e):
        open_unit(s, a, b, e)

        @pl.loop(0, blocks // UNROLL)
        def _(jj):
            for i in range(UNROLL):
                j = jj * UNROLL + i
                if a:
                    scores(s, u, j)
                if b:
                    powers((s - 1) % n_buf, j)
                if e:
                    context((s - 2) % n_buf, j)

        close_unit(s, u, a, b, e)

    group = CHUNKS // 2

    def o_slot(yy, f, g, lo, n):
        hh = half + f * (1 - 2 * half)
        return panel.at[pl.ds(g * group, group), pl.ds(lo, n), pl.ds(pl.multiple_of((CORES * yy + hh) * chunk, chunk), chunk)]

    def send_o(a, g):
        return pltpu.make_async_remote_copy(
            src_ref=obuf.at[pl.ds(g * group, group), pl.ds(a * Q_TILE, Q_TILE), :], dst_ref=o_slot(y, 0, g, a * Q_TILE, Q_TILE),
            send_sem=t_send.at[a, g], recv_sem=t_recv.at[a, g], device_id=far, device_id_type=MESH)

    def y_copy(f, a, g, way):
        piece = o_slot(y, f, g, a * Q_TILE, Q_TILE)
        return pltpu.make_async_remote_copy(src_ref=piece, dst_ref=piece, send_sem=y_send.at[f, a, g, way], recv_sem=y_recv.at[f, a, g, way], device_id=(up, down)[way], device_id_type=MESH)

    def y_pass(f, a, g, way):
        piece = o_slot((before, after)[way], f, g, a * Q_TILE + way * eighth, eighth)
        return pltpu.make_async_remote_copy(src_ref=piece, dst_ref=piece, send_sem=y_send.at[f, a, g, 2 + way], recv_sem=y_recv.at[f, a, g, 2 + way], device_id=(up, down)[way], device_id_type=MESH)

    def w_copy(kind, k):
        if kind == 0:
            return remote(w_slot(k, xn), w_slot(k, xn), f_send.at[k, 1], f_recv.at[k, 1], far)
        slot = w_slot(k, (x, xn, xf, xnf)[kind])
        return pltpu.make_async_remote_copy(src_ref=slot, dst_ref=slot, send_sem=d_send.at[k, kind], recv_sem=d_recv.at[k, kind], device_id=core, device_id_type=MESH)

    def near_in(k):
        to_near(k).wait_recv()
        if k >= 2:
            w_copy(0, k).start()
        w_copy(1, k).start()

    def far_in(k):
        to_far(k).wait_recv()
        w_copy(2, k).start()

    def corner_in(k):
        (corner(k) if k < 2 else w_copy(0, k)).wait_recv()
        w_copy(3, k).start()

    def y_start(f, a, g):
        for way in BOTH:
            y_copy(f, a, g, way).start()

    def y_relay(f, a, g):
        for way in BOTH:
            y_copy(f, a, g, way).wait_recv()
            y_pass(f, a, g, way).start()

    def o_in(a, g):
        send_o(a, g).wait_recv()
        y_start(1, a, g)

    def o_out(a, g):
        send_o(a, g).start()

    events = (
        (5, begin, to_near, 3), (6, begin, to_far, 3), (13, begin, to_near, 1), (22, begin, corner, 0), (29, begin, corner, 1),
        (7, o_out, 0, 0), (11, o_out, 0, 1), (12, near_in, 2), (12, far_in, 2),
        (15, o_out, 1, 0), (19, o_out, 1, 1), (19, o_in, 0, 0), (20, near_in, 3), (20, far_in, 3), (21, o_in, 0, 1),
        (22, y_relay, 1, 0, 0), (23, y_start, 0, 0, 0), (24, y_relay, 1, 0, 1), (28, near_in, 1),
        (26, y_relay, 0, 0, 0), (27, y_start, 0, 0, 1), (29, corner_in, 2), (30, y_relay, 0, 0, 1),
        (30, o_in, 1, 0), (31, y_start, 0, 1, 0),
    )

    unit(0, 0, YES, NO, NO)
    unit(1, 1, YES, YES, NO)

    @pl.loop(0, (units - 2) // n_buf)
    def _(i):
        for s in range(n_buf):
            for at in sorted({event[0] for event in events}):
                if (at - 2) % n_buf == s:
                    @pl.when(i == (at - 2) // n_buf)
                    def _(at=at):
                        for when, step, *which in events:
                            if when == at:
                                step(*which)
            unit((s + 2) % n_buf, 2 + i * n_buf + s, YES, YES, YES)

    unit(units % n_buf, units, NO, YES, YES)
    unit((units + 1) % n_buf, units + 1, NO, NO, YES)

    def multiply(a, k, first, last):
        tile = 2 * HEAD_DIM

        @pl.loop(0, width // tile)
        def _(n):
            cols = pl.ds(pl.multiple_of(n * tile, tile), tile)
            dot = jnp.dot(panel[k, pl.ds(a * Q_TILE, Q_TILE), :], wo[k, :, cols], preferred_element_type=jnp.float32)
            per = tile // 128
            if not first:
                dot = dot + jnp.concatenate([bufs[a][n * per + i] for i in range(per)], axis=1)
            if not last:
                for i in range(per):
                    bufs[a][n * per + i] = dot[:, i * 128:(i + 1) * 128]
            else:
                out_ref[pl.ds(a * Q_TILE, Q_TILE), cols] = dot.astype(jnp.bfloat16)

    def shares_in(k, kinds):
        for kind in kinds:
            w_copy(kind, k).wait_recv()

    def rows_in(a, g):
        for f in BOTH:
            for way in BOTH:
                y_pass(f, a, g, way).wait_recv()

    passed = (1, 2, 3)
    o_in(1, 1)
    y_start(0, 1, 1)
    y_relay(1, 1, 0)
    y_relay(0, 1, 0)
    corner_in(0)
    for copy in placed:
        copy.wait()
    for copy in shared:
        copy.wait_recv()
    rows_in(0, 0)
    rows_in(0, 1)
    shares_in(2, passed)
    multiply(0, 2, YES, NO)
    y_relay(1, 1, 1)
    y_relay(0, 1, 1)
    shares_in(0, passed[2:])
    multiply(0, 0, NO, NO)
    rows_in(1, 0)
    multiply(1, 0, YES, NO)
    rows_in(1, 1)
    multiply(1, 2, NO, NO)
    corner_in(3)
    corner_in(1)
    shares_in(3, passed)
    for a in BOTH:
        multiply(a, 3, NO, NO)
    shares_in(1, passed[::2])
    for a in BOTH:
        multiply(a, 1, NO, YES)
    for copy in started:
        copy.wait_send()
    to_near(1).wait_send()
    for k in BOTH:
        corner(k).wait_send()
    for k in (2, 3):
        to_near(k).wait_send()
        to_far(k).wait_send()
        w_copy(0, k).wait_send()
        for kind in (1, 2, 3):
            w_copy(kind, k).wait_send()
    for kind, k in ((3, 0), (1, 1), (3, 1)):
        w_copy(kind, k).wait_send()
    for a in BOTH:
        for g in BOTH:
            send_o(a, g).wait_send()
            for f in BOTH:
                for way in BOTH:
                    y_copy(f, a, g, way).wait_send()
                    y_pass(f, a, g, way).wait_send()


def attend_project(q, kv, segs, got, w_out, n_x, n_y):
    rows, ctx = q.shape[0] // 2, q.shape[1]
    keys = kv.shape[0]
    depth, width = w_out.shape
    n_row = CORES * n_x
    chunk = depth // CHUNKS
    dma = pltpu.SemaphoreType.DMA
    anywhere, vmem = pl.BlockSpec(memory_space=pl.ANY), pl.BlockSpec(memory_space=pltpu.VMEM)
    return pl.pallas_call(
        functools.partial(attend_kernel, n_x, n_y),
        out_shape=jax.ShapeDtypeStruct((rows, width), jnp.bfloat16),
        in_specs=[vmem, vmem, vmem, anywhere, anywhere],
        out_specs=vmem,
        scratch_shapes=[
            pltpu.VMEM((CHUNKS, n_row * chunk, width), jnp.bfloat16),
            pltpu.VMEM((CHUNKS, rows, n_row * chunk), jnp.bfloat16),
            pltpu.VMEM((CHUNKS, rows, chunk), jnp.bfloat16),
            pltpu.VMEM((keys // 128, Q_TILE, 128), jnp.float32),
            pltpu.VMEM((keys // 128, Q_TILE, 128), jnp.float32),
            pltpu.VMEM((keys // 128, Q_TILE, 128), jnp.float32),
            pltpu.VMEM((2 * rows, 128), jnp.float32),
            pltpu.VMEM((3, Q_TILE, 128), jnp.float32),
            pltpu.VMEM((3, Q_TILE, 128), jnp.float32),
            pltpu.VMEM((Q_TILE, HEAD_DIM), jnp.float32),
            *[dma(shape) for shape in ((CHUNKS, 2), (CHUNKS, 2), (CHUNKS, 4), (2, 2), (2, 2, 2, 4)) for _ in BOTH],
            dma((CHUNKS + 3,)),
        ],
        compiler_params=pltpu.CompilerParams(collective_id=1, has_side_effects=YES, vmem_limit_bytes=63 * 1024 * 1024),
        cost_estimate=pl.CostEstimate(flops=8 * rows * ctx * keys, bytes_accessed=4 * depth * width, transcendentals=0),
        name="attend_project",
    )(q, kv, segs, got, w_out)


def solution(mesh):
    n_x, n_y = mesh.shape["row"] // CORES, mesh.shape["col"]

    def local_block(tokens, w_qkv, w_out, doc_ids):
        q, kv, segs, got = project_qkv(tokens, w_qkv, w_out, doc_ids, n_x, n_y)
        return attend_project(q, kv, segs, got, w_out, n_x, n_y)

    row_spec = P(("data", "row"), "col")
    weight_spec = P("row", "col")
    return jax.shard_map(local_block, mesh=mesh, in_specs=(row_spec, weight_spec, weight_spec, P(("data", "row"))), out_specs=row_spec, check_vma=NO)
```

```python
import functools

import jax
import jax.numpy as jnp
from jax import lax
from jax.experimental import pallas as pl
from jax.experimental.pallas import tpu as pltpu
from jax.sharding import PartitionSpec as P

HEAD_DIM = 128
CORES = 2
Q_TILE = 256
CHUNKS = 4
UNROLL = 2
LOG2E = 1.4426950408889634
BOTH = (0, 1)
YES, NO = True, False


MESH = pl.DeviceIdType.MESH


def near_x(x):
    return x + 1 - 2 * (x % 2)


def qkv_kernel(n_x, n_y, tok_ref, w_ref, wo_ref, seg_ref, q_ref, kv_ref, segs_ref, got_ref, xg, wg, acc, w_send, w_recv, d_send, d_recv, t_send, t_recv, y_send, y_recv, k_send, k_recv, s_send, s_recv, o_send, o_recv, l_sem):
    r, y = lax.axis_index("row"), lax.axis_index("col")
    x, c = r // CORES, r % CORES
    xn, xf = near_x(x), n_x - 1 - x
    xnf = n_x - 1 - xn
    half = x // (n_x // 2)
    before, after, across = (y + n_y - 1) % n_y, (y + 1) % n_y, (y + 2) % n_y
    rows, width = tok_ref.shape
    depth = w_ref.shape[0]
    part = w_ref.shape[1] // 2
    ctx = part - 2 * HEAD_DIM
    mid, cut, quarter = rows // 2, depth // 2, rows // 4
    near, far, core = {"row": CORES * xn + c}, {"row": CORES * xf + c}, {"row": CORES * x + 1 - c}
    up, down = {"col": after}, {"col": before}

    barrier = pltpu.get_barrier_semaphore()
    n_row = CORES * n_x
    row_peers = [{"row": (r + d) % n_row} for d in range(1, n_row)]
    for peer in row_peers + [up, down]:
        pl.semaphore_signal(barrier, inc=1, device_id=peer, device_id_type=MESH)
    pl.semaphore_wait(barrier, n_row + 1)

    started = []

    def send(src, dst, s_sem, r_sem, peer):
        copy = pltpu.make_async_remote_copy(src_ref=src, dst_ref=dst, send_sem=s_sem, recv_sem=r_sem, device_id=peer, device_id_type=MESH)
        copy.start()
        started.append(copy)
        return copy

    mine = pl.ds(pl.multiple_of(half * part, 128), part)
    theirs = pl.ds(pl.multiple_of((1 - half) * part, 128), part)

    def w_slot(chip, plane, i):
        return wg.at[chip, pl.ds(pl.multiple_of(plane * depth + i * cut, cut), cut), :]

    def send_w(kind, i):
        src_rows = pl.ds(i * cut, cut)
        if kind == 0:
            return send(w_ref.at[src_rows, mine], w_slot(x, c, i), w_send.at[0, i], w_recv.at[0, i], near)
        if kind == 1:
            return send(w_ref.at[src_rows, theirs], w_slot(x, c, i), w_send.at[1, i], w_recv.at[1, i], far)
        return send(w_slot(xf, c, i), w_slot(xf, c, i), w_send.at[2, i], w_recv.at[2, i], near)

    def share(chip, i, at):
        src = w_ref.at[pl.ds(i * cut, cut), mine] if at == 0 else w_slot(chip, c, i)
        return send(src, w_slot(chip, c, i), d_send.at[at, i], d_recv.at[at, i], core)

    def x_slot(b, at, lo, n):
        return xg.at[b, at, pl.ds(lo, n), :]

    def send_t(a):
        return send(tok_ref.at[pl.ds(a * mid, mid), :], x_slot(1, y, a * mid, mid), t_send.at[a], t_recv.at[a], far)

    def send_y(b, a, way):
        src = tok_ref.at[pl.ds(a * mid, mid), :] if b == 0 else x_slot(1, y, a * mid, mid)
        return send(src, x_slot(b, y, a * mid, mid), y_send.at[b, a, way], y_recv.at[b, a, way], (up, down)[way])

    def pass_y(b, a, way):
        at = (before, after)[way]
        piece = x_slot(b, at, a * mid + way * quarter, quarter)
        return send(piece, piece, y_send.at[b, a, 2 + way], y_recv.at[b, a, 2 + way], (up, down)[way])

    segs = [send(seg_ref, segs_ref.at[r], s_send.at[d], s_recv.at[d], peer) for d, peer in enumerate(row_peers)]
    chunk = depth // CHUNKS

    def give_wo(i):
        return send(wo_ref.at[pl.ds(i * chunk, chunk), :], got_ref.at[1 + i], o_send.at[1 + i], o_recv.at[1 + i], far)

    w_far = [send_w(1, 0)]
    w_near = [send_w(0, 0)]
    y_own = [[send_y(0, 0, way) for way in BOTH]]
    locals_ = [
        pltpu.make_async_copy(seg_ref, segs_ref.at[r], l_sem.at[2]),
        pltpu.make_async_copy(tok_ref, xg.at[0, y], l_sem.at[0]),
        pltpu.make_async_copy(w_ref.at[:, mine], wg.at[x, pl.ds(pl.multiple_of(c * depth, depth), depth), :], l_sem.at[1]),
    ]
    for copy in locals_:
        copy.start()
    d_own = [share(x, i, 0) for i in BOTH]

    def multiply(b, lo, n, chip, first, last):
        tile = 2 * HEAD_DIM

        @pl.loop(0, part // tile)
        def _(j):
            cols = pl.ds(pl.multiple_of(j * tile, tile), tile)
            dot = jnp.dot(xg[b, chip, pl.ds(lo, n), :], wg[chip, :, cols], preferred_element_type=jnp.float32)
            if not first:
                dot = dot + acc[pl.ds(lo, n), cols]
            if not last:
                acc[pl.ds(lo, n), cols] = dot
            else:
                out = dot.astype(jnp.bfloat16)

                @pl.when(j < ctx // tile)
                def _():
                    q_ref[pl.ds(b * rows + lo, n), cols] = out

                @pl.when(j == ctx // tile)
                def _():
                    kv_ref[pl.ds(b * rows + lo, n), :] = out

    def kv_slot(s):
        return kv_ref.at[pl.ds(s * rows, rows), :]

    def kv_near(b):
        return send(kv_slot(b), kv_slot(2 + b), k_send.at[b], k_recv.at[b], near)

    def kv_core(s):
        return send(kv_slot(s), kv_slot(4 + s), k_send.at[2 + s], k_recv.at[2 + s], core)

    def relay(b, a):
        got = []
        for way in BOTH:
            (y_own if b == 0 else y_par)[a][way].wait_recv()
            got.append(pass_y(b, a, way))
        return got

    y_far = [relay(0, 0)]
    y_own.append([send_y(0, 1, way) for way in BOTH])
    tok = [send_t(0)]
    w_near.append(send_w(0, 1))
    w_near[0].wait_recv()
    d_near = [share(xn, 0, 1)]
    w_far[0].wait_recv()
    w_nf = [send_w(2, 0)]
    d_far = [share(xf, 0, 2)]
    tok[0].wait_recv()
    w_far.append(send_w(1, 1))
    y_par = [[send_y(1, 0, way) for way in BOTH]]
    y_far.append(relay(0, 1))
    w_near[1].wait_recv()
    d_near.append(share(xn, 1, 1))
    for pair in y_far:
        for copy in pair:
            copy.wait_recv()
    for copy in locals_:
        copy.wait()
    for copy in d_own:
        copy.wait_recv()
    multiply(0, 0, rows, x, YES, NO)
    tok.append(send_t(1))
    for copy in d_near:
        copy.wait_recv()
    multiply(0, 0, rows, xn, NO, NO)
    w_far[1].wait_recv()
    w_nf.append(send_w(2, 1))
    d_far.append(share(xf, 1, 2))
    y_pfar = [relay(1, 0)]
    w_nf[0].wait_recv()
    d_nf = [share(xnf, 0, 3)]
    for copy in d_far:
        copy.wait_recv()
    multiply(0, 0, rows, xf, NO, NO)
    tok[1].wait_recv()
    y_par.append([send_y(1, 1, way) for way in BOTH])
    wo_got = [give_wo(0)]
    w_nf[1].wait_recv()
    wo_got.append(send(wo_ref.at[pl.ds(0, chunk), :], got_ref.at[0], o_send.at[0], o_recv.at[0], near))
    wo_got.append(give_wo(1))
    d_nf.append(share(xnf, 1, 3))
    for copy in d_nf:
        copy.wait_recv()
    multiply(0, 0, rows, xnf, NO, YES)
    for copy in y_pfar[0]:
        copy.wait_recv()
    multiply(1, 0, mid, y, YES, NO)
    k_near, k_core = [kv_near(0)], [kv_core(0)]
    multiply(1, 0, mid, before, NO, NO)
    y_pfar.append(relay(1, 1))
    multiply(1, 0, mid, after, NO, NO)
    multiply(1, 0, mid, across, NO, YES)
    multiply(1, mid, mid, y, YES, NO)
    multiply(1, mid, mid, before, NO, NO)
    multiply(1, mid, mid, after, NO, NO)
    k_near[0].wait_recv()
    k_core.append(kv_core(2))
    for copy in y_pfar[1]:
        copy.wait_recv()
    multiply(1, mid, mid, across, NO, YES)
    k_near.append(kv_near(1))
    k_core.append(kv_core(1))
    k_near[1].wait_recv()
    k_core.append(kv_core(3))
    for copy in k_core + wo_got + segs:
        copy.wait_recv()
    for copy in started:
        copy.wait_send()


def project_qkv(tokens, w_qkv, w_out, doc_ids, n_x, n_y):
    rows, width = tokens.shape
    depth, cols = w_qkv.shape
    part = cols // 2
    ctx = part - 2 * HEAD_DIM
    n_row = CORES * n_x
    dma = pltpu.SemaphoreType.DMA
    anywhere, vmem = pl.BlockSpec(memory_space=pl.ANY), pl.BlockSpec(memory_space=pltpu.VMEM)
    segs = doc_ids.reshape(rows // 128, 128)
    return pl.pallas_call(
        functools.partial(qkv_kernel, n_x, n_y),
        out_shape=(
            jax.ShapeDtypeStruct((2 * rows, ctx), jnp.bfloat16),
            jax.ShapeDtypeStruct((n_row * rows, 2 * HEAD_DIM), jnp.bfloat16),
            jax.ShapeDtypeStruct((n_row,) + segs.shape, jnp.int32),
            jax.ShapeDtypeStruct((3, depth // CHUNKS, w_out.shape[1]), jnp.bfloat16),
        ),
        in_specs=[anywhere] * 4,
        out_specs=(vmem, vmem, vmem, anywhere),
        scratch_shapes=[
            pltpu.VMEM((2, n_y, rows, width), jnp.bfloat16),
            pltpu.VMEM((n_x, CORES * depth, part), jnp.bfloat16),
            pltpu.VMEM((rows, part), jnp.float32),
            *[dma(shape) for shape in ((3, 2), (4, 2), (2,), (2, 2, 4), (6,), (n_row - 1,), (3,)) for _ in BOTH],
            dma((3,)),
        ],
        compiler_params=pltpu.CompilerParams(collective_id=0, has_side_effects=YES, vmem_limit_bytes=60 * 1024 * 1024),
        cost_estimate=pl.CostEstimate(flops=4 * rows * n_y * width * part, bytes_accessed=2 * depth * cols, transcendentals=0),
        name="project_qkv",
    )(tokens, w_qkv, w_out, segs)


def attend_kernel(n_x, n_y, q_ref, kv_ref, segs_ref, got_ref, w_ref, out_ref, wo, panel, obuf, buf_a, buf_b, buf_c, segq, mbuf, lbuf, abuf, n_send, n_recv, f_send, f_recv, d_send, d_recv, t_send, t_recv, y_send, y_recv, l_sem):
    r, y = lax.axis_index("row"), lax.axis_index("col")
    x, c = r // CORES, r % CORES
    xn, xf = near_x(x), n_x - 1 - x
    xnf = n_x - 1 - xn
    half = x // (n_x // 2)
    before, after, across = (y + n_y - 1) % n_y, (y + 1) % n_y, (y + 2) % n_y
    rows = out_ref.shape[0]
    keys = kv_ref.shape[0]
    chunk = w_ref.shape[0] // CHUNKS
    width = w_ref.shape[1]
    heads = q_ref.shape[1] // HEAD_DIM
    tiles = 2 * rows // Q_TILE
    units = tiles * heads
    eighth = Q_TILE // 2
    coef = HEAD_DIM ** -0.5 * LOG2E
    lowest = jnp.finfo(jnp.float32).min
    near, far, core = {"row": CORES * xn + c}, {"row": CORES * xf + c}, {"row": CORES * x + 1 - c}
    up, down = {"col": after}, {"col": before}

    barrier = pltpu.get_barrier_semaphore()
    for peer in (near, far, core, up, down):
        pl.semaphore_signal(barrier, inc=1, device_id=peer, device_id_type=MESH)
    pl.semaphore_wait(barrier, 5)

    started = []

    def send(src, dst, s_sem, r_sem, peer):
        copy = pltpu.make_async_remote_copy(src_ref=src, dst_ref=dst, send_sem=s_sem, recv_sem=r_sem, device_id=peer, device_id_type=MESH)
        copy.start()
        started.append(copy)
        return copy

    def w_slot(k, chip):
        return wo.at[k, pl.ds(pl.multiple_of((CORES * chip + c) * chunk, chunk), chunk), :]

    def w_mine(k):
        return w_ref.at[pl.ds(k * chunk, chunk), :]

    def share(k, origin, src=None):
        slot = w_slot(k, (x, xn, xf, xnf)[origin])
        return send(slot if src is None else src, slot, d_send.at[k, origin], d_recv.at[k, origin], core)

    def remote(src, dst, s_sem, r_sem, peer):
        return pltpu.make_async_remote_copy(src_ref=src, dst_ref=dst, send_sem=s_sem, recv_sem=r_sem, device_id=peer, device_id_type=MESH)

    def to_near(k):
        return remote(w_mine(k), w_slot(k, x), n_send.at[k, 0], n_recv.at[k, 0], near)

    def to_far(k):
        return remote(w_mine(k), w_slot(k, x), f_send.at[k, 0], f_recv.at[k, 0], far)

    def corner(k):
        return remote(got_ref.at[1 + k], w_slot(k, xf), n_send.at[k, 1], n_recv.at[k, 1], near)

    def begin(copy, k):
        copy(k).start()

    begin(to_near, 2)
    begin(to_far, 2)
    places = [(w_mine(k), w_slot(k, x)) for k in range(CHUNKS)]
    places += [(got_ref.at[0], w_slot(0, xn)), (got_ref.at[1], w_slot(0, xf)), (got_ref.at[2], w_slot(1, xf))]
    placed = [pltpu.make_async_copy(src, dst, l_sem.at[i]) for i, (src, dst) in enumerate(places)]
    for copy in placed:
        copy.start()
    shared = [share(k, 0, w_mine(k)) for k in range(CHUNKS)]
    shared += [share(0, 1, got_ref.at[0]), share(0, 2, got_ref.at[1]), share(1, 2, got_ref.at[2])]

    for i in range(2 * rows // 128):
        at = r if i < rows // 128 else CORES * xf + c
        line = segs_ref[at, pl.ds(i % (rows // 128), 1), :].astype(jnp.float32)
        segq[pl.ds(i * 128, 128), :] = jnp.broadcast_to(line, (128, 128)).T

    def key_row(j):
        odd, fam, plane = j % 2, (j // 2) % 2, j // 4
        base = x + fam * (xn - x)
        chip = base + odd * (n_x - 1 - 2 * base)
        return CORES * chip + c + plane * (1 - 2 * c)

    blocks = keys // rows
    lanes = rows // 128
    bufs = (buf_a, buf_b, buf_c)
    n_buf = len(bufs)

    def scores(b, u, j):
        tile, h = (u // heads + tiles // 2) % tiles, u % heads
        q = q_ref[pl.ds(pl.multiple_of(tile * Q_TILE, Q_TILE), Q_TILE), pl.ds(pl.multiple_of(h * HEAD_DIM, HEAD_DIM), HEAD_DIM)]
        k = kv_ref[pl.ds(pl.multiple_of(j * rows, rows), rows), pl.ds(0, HEAD_DIM)]
        s = lax.dot_general(q, k, (((1,), (1,)), ((), ())), preferred_element_type=jnp.float32)
        own = segq[pl.ds(pl.multiple_of(tile * Q_TILE, Q_TILE), Q_TILE), :]
        seg = segs_ref[key_row(j)].astype(jnp.float32)
        top = mbuf[b]
        for i in range(lanes):
            part = jnp.where(own == seg[i:i + 1, :], s[:, i * 128:(i + 1) * 128], lowest)
            bufs[b][j * lanes + i] = part
            top = jnp.maximum(top, part)
        mbuf[b] = top

    def powers(b, j):
        top = mbuf[b]
        total = lbuf[b]
        for i in range(lanes):
            e = jnp.exp2((bufs[b][j * lanes + i] - top) * coef)
            bufs[b][j * lanes + i] = e
            total = total + e
        lbuf[b] = total

    def context(b, j):
        inv = lbuf[b]
        p = jnp.concatenate([(bufs[b][j * lanes + i] * inv).astype(jnp.bfloat16) for i in range(lanes)], axis=1)
        v = kv_ref[pl.ds(pl.multiple_of(j * rows, rows), rows), pl.ds(HEAD_DIM, HEAD_DIM)]
        abuf[...] += jnp.dot(p, v, preferred_element_type=jnp.float32)

    def open_unit(s, a, b, e):
        if a:
            mbuf[s] = jnp.full(mbuf.shape[1:], lowest, jnp.float32)
        if b:
            lbuf[(s - 1) % n_buf] = jnp.zeros(lbuf.shape[1:], jnp.float32)
        if e:
            abuf[...] = jnp.zeros(abuf.shape, jnp.float32)

    def close_unit(s, u, a, b, e):
        if a:
            mbuf[s] = jnp.broadcast_to(jnp.max(mbuf[s], axis=1, keepdims=YES), mbuf.shape[1:])
        if b:
            lbuf[(s - 1) % n_buf] = 1.0 / jnp.broadcast_to(jnp.sum(lbuf[(s - 1) % n_buf], axis=1, keepdims=YES), lbuf.shape[1:])
        if e:
            tile, h = (u - 2) // heads, (u - 2) % heads
            out = abuf[...].astype(jnp.bfloat16)
            per = heads // CHUNKS
            lo = pl.multiple_of((h % per) * HEAD_DIM, HEAD_DIM)
            mine = pl.multiple_of((CORES * y + half) * chunk, chunk)

            at = pl.ds(pl.multiple_of(tile % (tiles // 2) * Q_TILE, Q_TILE), Q_TILE)

            @pl.when(tile >= tiles // 2)
            def _():
                panel[h // per, at, pl.ds(pl.multiple_of(mine + lo, HEAD_DIM), HEAD_DIM)] = out

            @pl.when(tile < tiles // 2)
            def _():
                obuf[h // per, at, pl.ds(lo, HEAD_DIM)] = out

    def unit(s, u, a, b, e):
        open_unit(s, a, b, e)

        @pl.loop(0, blocks // UNROLL)
        def _(jj):
            for i in range(UNROLL):
                j = jj * UNROLL + i
                if a:
                    scores(s, u, j)
                if b:
                    powers((s - 1) % n_buf, j)
                if e:
                    context((s - 2) % n_buf, j)

        close_unit(s, u, a, b, e)

    group = CHUNKS // 2

    def o_slot(yy, f, g, lo, n):
        hh = half + f * (1 - 2 * half)
        return panel.at[pl.ds(g * group, group), pl.ds(lo, n), pl.ds(pl.multiple_of((CORES * yy + hh) * chunk, chunk), chunk)]

    def send_o(a, g):
        return pltpu.make_async_remote_copy(
            src_ref=obuf.at[pl.ds(g * group, group), pl.ds(a * Q_TILE, Q_TILE), :], dst_ref=o_slot(y, 0, g, a * Q_TILE, Q_TILE),
            send_sem=t_send.at[a, g], recv_sem=t_recv.at[a, g], device_id=far, device_id_type=MESH)

    def y_copy(f, a, g, way):
        piece = o_slot(y, f, g, a * Q_TILE, Q_TILE)
        return pltpu.make_async_remote_copy(src_ref=piece, dst_ref=piece, send_sem=y_send.at[f, a, g, way], recv_sem=y_recv.at[f, a, g, way], device_id=(up, down)[way], device_id_type=MESH)

    def y_pass(f, a, g, way):
        piece = o_slot((before, after)[way], f, g, a * Q_TILE + way * eighth, eighth)
        return pltpu.make_async_remote_copy(src_ref=piece, dst_ref=piece, send_sem=y_send.at[f, a, g, 2 + way], recv_sem=y_recv.at[f, a, g, 2 + way], device_id=(up, down)[way], device_id_type=MESH)

    def w_copy(kind, k):
        if kind == 0:
            return remote(w_slot(k, xn), w_slot(k, xn), f_send.at[k, 1], f_recv.at[k, 1], far)
        slot = w_slot(k, (x, xn, xf, xnf)[kind])
        return pltpu.make_async_remote_copy(src_ref=slot, dst_ref=slot, send_sem=d_send.at[k, kind], recv_sem=d_recv.at[k, kind], device_id=core, device_id_type=MESH)

    def near_in(k):
        to_near(k).wait_recv()
        if k >= 2:
            w_copy(0, k).start()
        w_copy(1, k).start()

    def far_in(k):
        to_far(k).wait_recv()
        w_copy(2, k).start()

    def corner_in(k):
        (corner(k) if k < 2 else w_copy(0, k)).wait_recv()
        w_copy(3, k).start()

    def y_start(f, a, g):
        for way in BOTH:
            y_copy(f, a, g, way).start()

    def y_relay(f, a, g):
        for way in BOTH:
            y_copy(f, a, g, way).wait_recv()
            y_pass(f, a, g, way).start()

    def o_in(a, g):
        send_o(a, g).wait_recv()
        y_start(1, a, g)

    def o_out(a, g):
        send_o(a, g).start()

    events = (
        (5, begin, to_near, 3), (7, o_out, 0, 0), (8, begin, to_far, 3), (11, o_out, 0, 1), (13, begin, to_near, 1),
        (15, o_out, 1, 0), (19, o_out, 1, 1), (19, o_in, 0, 0), (20, near_in, 2), (20, far_in, 2), (21, o_in, 0, 1),
        (22, begin, corner, 0), (23, y_relay, 1, 0, 0), (23, y_start, 0, 0, 0), (25, y_relay, 1, 0, 1),
        (27, y_relay, 0, 0, 0), (27, y_start, 0, 0, 1), (28, near_in, 3), (28, far_in, 3), (28, near_in, 1),
        (29, begin, corner, 1), (29, o_in, 1, 0), (31, y_relay, 0, 0, 1), (31, y_start, 0, 1, 0),
    )

    unit(0, 0, YES, NO, NO)
    unit(1, 1, YES, YES, NO)

    @pl.loop(0, (units - 2) // n_buf)
    def _(i):
        for s in range(n_buf):
            for at in sorted({event[0] for event in events}):
                if (at - 2) % n_buf == s:
                    @pl.when(i == (at - 2) // n_buf)
                    def _(at=at):
                        for when, step, *which in events:
                            if when == at:
                                step(*which)
            unit((s + 2) % n_buf, 2 + i * n_buf + s, YES, YES, YES)

    unit(units % n_buf, units, NO, YES, YES)
    unit((units + 1) % n_buf, units + 1, NO, NO, YES)

    def multiply(a, k, first, last):
        tile = 2 * HEAD_DIM

        @pl.loop(0, width // tile)
        def _(n):
            cols = pl.ds(pl.multiple_of(n * tile, tile), tile)
            dot = jnp.dot(panel[k, pl.ds(a * Q_TILE, Q_TILE), :], wo[k, :, cols], preferred_element_type=jnp.float32)
            per = tile // 128
            if not first:
                dot = dot + jnp.concatenate([bufs[a][n * per + i] for i in range(per)], axis=1)
            if not last:
                for i in range(per):
                    bufs[a][n * per + i] = dot[:, i * 128:(i + 1) * 128]
            else:
                out_ref[pl.ds(a * Q_TILE, Q_TILE), cols] = dot.astype(jnp.bfloat16)

    def shares_in(k, kinds):
        for kind in kinds:
            w_copy(kind, k).wait_recv()

    def rows_in(a, g):
        for f in BOTH:
            for way in BOTH:
                y_pass(f, a, g, way).wait_recv()

    passed = (1, 2, 3)
    o_in(1, 1)
    y_start(0, 1, 1)
    y_relay(1, 1, 0)
    y_relay(0, 1, 0)
    corner_in(2)
    corner_in(0)
    for copy in placed:
        copy.wait()
    for copy in shared:
        copy.wait_recv()
    rows_in(0, 0)
    rows_in(0, 1)
    shares_in(2, passed)
    multiply(0, 2, YES, NO)
    y_relay(1, 1, 1)
    y_relay(0, 1, 1)
    shares_in(0, passed[2:])
    multiply(0, 0, NO, NO)
    rows_in(1, 0)
    multiply(1, 0, YES, NO)
    rows_in(1, 1)
    multiply(1, 2, NO, NO)
    corner_in(3)
    shares_in(3, passed)
    multiply(0, 3, NO, NO)
    corner_in(1)
    multiply(1, 3, NO, NO)
    shares_in(1, passed[::2])
    for a in BOTH:
        multiply(a, 1, NO, YES)
    for copy in started:
        copy.wait_send()
    to_near(1).wait_send()
    for k in BOTH:
        corner(k).wait_send()
    for k in (2, 3):
        to_near(k).wait_send()
        to_far(k).wait_send()
        w_copy(0, k).wait_send()
        for kind in (1, 2, 3):
            w_copy(kind, k).wait_send()
    for kind, k in ((3, 0), (1, 1), (3, 1)):
        w_copy(kind, k).wait_send()
    for a in BOTH:
        for g in BOTH:
            send_o(a, g).wait_send()
            for f in BOTH:
                for way in BOTH:
                    y_copy(f, a, g, way).wait_send()
                    y_pass(f, a, g, way).wait_send()


def attend_project(q, kv, segs, got, w_out, n_x, n_y):
    rows, ctx = q.shape[0] // 2, q.shape[1]
    keys = kv.shape[0]
    depth, width = w_out.shape
    n_row = CORES * n_x
    chunk = depth // CHUNKS
    dma = pltpu.SemaphoreType.DMA
    anywhere, vmem = pl.BlockSpec(memory_space=pl.ANY), pl.BlockSpec(memory_space=pltpu.VMEM)
    return pl.pallas_call(
        functools.partial(attend_kernel, n_x, n_y),
        out_shape=jax.ShapeDtypeStruct((rows, width), jnp.bfloat16),
        in_specs=[vmem, vmem, vmem, anywhere, anywhere],
        out_specs=vmem,
        scratch_shapes=[
            pltpu.VMEM((CHUNKS, n_row * chunk, width), jnp.bfloat16),
            pltpu.VMEM((CHUNKS, rows, n_row * chunk), jnp.bfloat16),
            pltpu.VMEM((CHUNKS, rows, chunk), jnp.bfloat16),
            pltpu.VMEM((keys // 128, Q_TILE, 128), jnp.float32),
            pltpu.VMEM((keys // 128, Q_TILE, 128), jnp.float32),
            pltpu.VMEM((keys // 128, Q_TILE, 128), jnp.float32),
            pltpu.VMEM((2 * rows, 128), jnp.float32),
            pltpu.VMEM((3, Q_TILE, 128), jnp.float32),
            pltpu.VMEM((3, Q_TILE, 128), jnp.float32),
            pltpu.VMEM((Q_TILE, HEAD_DIM), jnp.float32),
            *[dma(shape) for shape in ((CHUNKS, 2), (CHUNKS, 2), (CHUNKS, 4), (2, 2), (2, 2, 2, 4)) for _ in BOTH],
            dma((CHUNKS + 3,)),
        ],
        compiler_params=pltpu.CompilerParams(collective_id=1, has_side_effects=YES, vmem_limit_bytes=63 * 1024 * 1024),
        cost_estimate=pl.CostEstimate(flops=8 * rows * ctx * keys, bytes_accessed=4 * depth * width, transcendentals=0),
        name="attend_project",
    )(q, kv, segs, got, w_out)


def solution(mesh):
    n_x, n_y = mesh.shape["row"] // CORES, mesh.shape["col"]

    def local_block(tokens, w_qkv, w_out, doc_ids):
        q, kv, segs, got = project_qkv(tokens, w_qkv, w_out, doc_ids, n_x, n_y)
        return attend_project(q, kv, segs, got, w_out, n_x, n_y)

    row_spec = P(("data", "row"), "col")
    weight_spec = P("row", "col")
    return jax.shard_map(local_block, mesh=mesh, in_specs=(row_spec, weight_spec, weight_spec, P(("data", "row"))), out_specs=row_spec, check_vma=NO)
```

```python
import functools

import jax
import jax.numpy as jnp
from jax import lax
from jax.experimental import pallas as pl
from jax.experimental.pallas import tpu as pltpu
from jax.sharding import PartitionSpec as P

HEAD_DIM = 128
CORES = 2
Q_TILE = 256
CHUNKS = 4
UNROLL = 2
LOG2E = 1.4426950408889634
BOTH = (0, 1)
YES, NO = True, False


MESH = pl.DeviceIdType.MESH


def near_x(x):
    return x + 1 - 2 * (x % 2)


def qkv_kernel(n_x, n_y, tok_ref, w_ref, wo_ref, seg_ref, q_ref, kv_ref, segs_ref, got_ref, xg, wg, acc, w_send, w_recv, d_send, d_recv, t_send, t_recv, y_send, y_recv, k_send, k_recv, s_send, s_recv, o_send, o_recv, l_sem):
    r, y = lax.axis_index("row"), lax.axis_index("col")
    x, c = r // CORES, r % CORES
    xn, xf = near_x(x), n_x - 1 - x
    xnf = n_x - 1 - xn
    half = x // (n_x // 2)
    before, after, across = (y + n_y - 1) % n_y, (y + 1) % n_y, (y + 2) % n_y
    rows, width = tok_ref.shape
    depth = w_ref.shape[0]
    part = w_ref.shape[1] // 2
    ctx = part - 2 * HEAD_DIM
    mid, cut, quarter = rows // 2, depth // 2, rows // 4
    near, far, core = {"row": CORES * xn + c}, {"row": CORES * xf + c}, {"row": CORES * x + 1 - c}
    up, down = {"col": after}, {"col": before}

    barrier = pltpu.get_barrier_semaphore()
    n_row = CORES * n_x
    row_peers = [{"row": (r + d) % n_row} for d in range(1, n_row)]
    for peer in row_peers + [up, down]:
        pl.semaphore_signal(barrier, inc=1, device_id=peer, device_id_type=MESH)
    pl.semaphore_wait(barrier, n_row + 1)

    started = []

    def send(src, dst, s_sem, r_sem, peer):
        copy = pltpu.make_async_remote_copy(src_ref=src, dst_ref=dst, send_sem=s_sem, recv_sem=r_sem, device_id=peer, device_id_type=MESH)
        copy.start()
        started.append(copy)
        return copy

    mine = pl.ds(pl.multiple_of(half * part, 128), part)
    theirs = pl.ds(pl.multiple_of((1 - half) * part, 128), part)

    def w_slot(chip, plane, i):
        return wg.at[chip, pl.ds(pl.multiple_of(plane * depth + i * cut, cut), cut), :]

    def send_w(kind, i):
        src_rows = pl.ds(i * cut, cut)
        if kind == 0:
            return send(w_ref.at[src_rows, mine], w_slot(x, c, i), w_send.at[0, i], w_recv.at[0, i], near)
        if kind == 1:
            return send(w_ref.at[src_rows, theirs], w_slot(x, c, i), w_send.at[1, i], w_recv.at[1, i], far)
        return send(w_slot(xf, c, i), w_slot(xf, c, i), w_send.at[2, i], w_recv.at[2, i], near)

    def share(chip, i, at):
        src = w_ref.at[pl.ds(i * cut, cut), mine] if at == 0 else w_slot(chip, c, i)
        return send(src, w_slot(chip, c, i), d_send.at[at, i], d_recv.at[at, i], core)

    def x_slot(b, at, lo, n):
        return xg.at[b, at, pl.ds(lo, n), :]

    def send_t(a):
        return send(tok_ref.at[pl.ds(a * mid, mid), :], x_slot(1, y, a * mid, mid), t_send.at[a], t_recv.at[a], far)

    def send_y(b, a, way):
        src = tok_ref.at[pl.ds(a * mid, mid), :] if b == 0 else x_slot(1, y, a * mid, mid)
        return send(src, x_slot(b, y, a * mid, mid), y_send.at[b, a, way], y_recv.at[b, a, way], (up, down)[way])

    def pass_y(b, a, way):
        at = (before, after)[way]
        piece = x_slot(b, at, a * mid + way * quarter, quarter)
        return send(piece, piece, y_send.at[b, a, 2 + way], y_recv.at[b, a, 2 + way], (up, down)[way])

    segs = [send(seg_ref, segs_ref.at[r], s_send.at[d], s_recv.at[d], peer) for d, peer in enumerate(row_peers)]
    w_far = [send_w(1, 0)]
    y_own = [[send_y(0, a, way) for way in BOTH] for a in BOTH]
    w_near = [send_w(0, 0)]
    tok = [send_t(0)]
    w_near.append(send_w(0, 1))
    w_far.append(send_w(1, 1))
    tok.append(send_t(1))
    chunk = depth // CHUNKS
    locals_ = [
        pltpu.make_async_copy(seg_ref, segs_ref.at[r], l_sem.at[2]),
        pltpu.make_async_copy(tok_ref, xg.at[0, y], l_sem.at[0]),
        pltpu.make_async_copy(w_ref.at[:, mine], wg.at[x, pl.ds(pl.multiple_of(c * depth, depth), depth), :], l_sem.at[1]),
    ]
    for copy in locals_:
        copy.start()
    d_own = [share(x, i, 0) for i in BOTH]

    def multiply(b, lo, n, chip, first, last):
        tile = 2 * HEAD_DIM

        @pl.loop(0, part // tile)
        def _(j):
            cols = pl.ds(pl.multiple_of(j * tile, tile), tile)
            dot = jnp.dot(xg[b, chip, pl.ds(lo, n), :], wg[chip, :, cols], preferred_element_type=jnp.float32)
            if not first:
                dot = dot + acc[pl.ds(lo, n), cols]
            if not last:
                acc[pl.ds(lo, n), cols] = dot
            else:
                out = dot.astype(jnp.bfloat16)

                @pl.when(j < ctx // tile)
                def _():
                    q_ref[pl.ds(b * rows + lo, n), cols] = out

                @pl.when(j == ctx // tile)
                def _():
                    kv_ref[pl.ds(b * rows + lo, n), :] = out

    def kv_slot(s):
        return kv_ref.at[pl.ds(s * rows, rows), :]

    def kv_near(b):
        return send(kv_slot(b), kv_slot(2 + b), k_send.at[b], k_recv.at[b], near)

    def kv_core(s):
        return send(kv_slot(s), kv_slot(4 + s), k_send.at[2 + s], k_recv.at[2 + s], core)

    def relay(b, a):
        got = []
        for way in BOTH:
            (y_own if b == 0 else y_par)[a][way].wait_recv()
            got.append(pass_y(b, a, way))
        return got

    y_far = [relay(0, 0)]
    w_far[0].wait_recv()
    w_nf = [send_w(2, 0)]
    d_far = [share(xf, 0, 2)]
    w_near[0].wait_recv()
    d_near = [share(xn, 0, 1)]
    y_far.append(relay(0, 1))
    tok[0].wait_recv()
    y_par = [[send_y(1, 0, way) for way in BOTH]]
    wo_got = [send(wo_ref.at[pl.ds(i * chunk, chunk), :], got_ref.at[1 + i], o_send.at[1 + i], o_recv.at[1 + i], far) for i in BOTH]
    w_near[1].wait_recv()
    d_near.append(share(xn, 1, 1))
    for pair in y_far:
        for copy in pair:
            copy.wait_recv()
    for copy in locals_:
        copy.wait()
    for copy in d_own:
        copy.wait_recv()
    multiply(0, 0, rows, x, YES, NO)
    for copy in d_near:
        copy.wait_recv()
    w_far[1].wait_recv()
    w_nf.append(send_w(2, 1))
    wo_got.append(send(wo_ref.at[pl.ds(0, chunk), :], got_ref.at[0], o_send.at[0], o_recv.at[0], near))
    d_far.append(share(xf, 1, 2))
    multiply(0, 0, rows, xn, NO, NO)
    w_nf[0].wait_recv()
    d_nf = [share(xnf, 0, 3)]
    y_pfar = [relay(1, 0)]
    tok[1].wait_recv()
    y_par.append([send_y(1, 1, way) for way in BOTH])
    for copy in d_far:
        copy.wait_recv()
    multiply(0, 0, rows, xf, NO, NO)
    w_nf[1].wait_recv()
    d_nf.append(share(xnf, 1, 3))
    for copy in d_nf:
        copy.wait_recv()
    multiply(0, 0, rows, xnf, NO, YES)
    for copy in y_pfar[0]:
        copy.wait_recv()
    multiply(1, 0, mid, y, YES, NO)
    k_near, k_core = [kv_near(0)], [kv_core(0)]
    multiply(1, 0, mid, before, NO, NO)
    y_pfar.append(relay(1, 1))
    multiply(1, 0, mid, after, NO, NO)
    multiply(1, 0, mid, across, NO, YES)
    multiply(1, mid, mid, y, YES, NO)
    multiply(1, mid, mid, before, NO, NO)
    multiply(1, mid, mid, after, NO, NO)
    k_near[0].wait_recv()
    k_core.append(kv_core(2))
    for copy in y_pfar[1]:
        copy.wait_recv()
    multiply(1, mid, mid, across, NO, YES)
    k_near.append(kv_near(1))
    k_core.append(kv_core(1))
    k_near[1].wait_recv()
    k_core.append(kv_core(3))
    for copy in k_core + wo_got + segs:
        copy.wait_recv()
    for copy in started:
        copy.wait_send()


def project_qkv(tokens, w_qkv, w_out, doc_ids, n_x, n_y):
    rows, width = tokens.shape
    depth, cols = w_qkv.shape
    part = cols // 2
    ctx = part - 2 * HEAD_DIM
    n_row = CORES * n_x
    dma = pltpu.SemaphoreType.DMA
    anywhere, vmem = pl.BlockSpec(memory_space=pl.ANY), pl.BlockSpec(memory_space=pltpu.VMEM)
    segs = doc_ids.reshape(rows // 128, 128)
    return pl.pallas_call(
        functools.partial(qkv_kernel, n_x, n_y),
        out_shape=(
            jax.ShapeDtypeStruct((2 * rows, ctx), jnp.bfloat16),
            jax.ShapeDtypeStruct((n_row * rows, 2 * HEAD_DIM), jnp.bfloat16),
            jax.ShapeDtypeStruct((n_row,) + segs.shape, jnp.int32),
            jax.ShapeDtypeStruct((3, depth // CHUNKS, w_out.shape[1]), jnp.bfloat16),
        ),
        in_specs=[anywhere] * 4,
        out_specs=(vmem, vmem, vmem, anywhere),
        scratch_shapes=[
            pltpu.VMEM((2, n_y, rows, width), jnp.bfloat16),
            pltpu.VMEM((n_x, CORES * depth, part), jnp.bfloat16),
            pltpu.VMEM((rows, part), jnp.float32),
            *[dma(shape) for shape in ((3, 2), (4, 2), (2,), (2, 2, 4), (6,), (n_row - 1,), (3,)) for _ in BOTH],
            dma((3,)),
        ],
        compiler_params=pltpu.CompilerParams(collective_id=0, has_side_effects=YES, vmem_limit_bytes=60 * 1024 * 1024),
        cost_estimate=pl.CostEstimate(flops=4 * rows * n_y * width * part, bytes_accessed=2 * depth * cols, transcendentals=0),
        name="project_qkv",
    )(tokens, w_qkv, w_out, segs)


def attend_kernel(n_x, n_y, q_ref, kv_ref, segs_ref, got_ref, w_ref, out_ref, wo, panel, obuf, buf_a, buf_b, buf_c, segq, mbuf, lbuf, abuf, n_send, n_recv, f_send, f_recv, d_send, d_recv, t_send, t_recv, y_send, y_recv, l_sem):
    r, y = lax.axis_index("row"), lax.axis_index("col")
    x, c = r // CORES, r % CORES
    xn, xf = near_x(x), n_x - 1 - x
    xnf = n_x - 1 - xn
    half = x // (n_x // 2)
    before, after, across = (y + n_y - 1) % n_y, (y + 1) % n_y, (y + 2) % n_y
    rows = out_ref.shape[0]
    keys = kv_ref.shape[0]
    chunk = w_ref.shape[0] // CHUNKS
    width = w_ref.shape[1]
    heads = q_ref.shape[1] // HEAD_DIM
    tiles = 2 * rows // Q_TILE
    units = tiles * heads
    eighth = Q_TILE // 2
    coef = HEAD_DIM ** -0.5 * LOG2E
    lowest = jnp.finfo(jnp.float32).min
    near, far, core = {"row": CORES * xn + c}, {"row": CORES * xf + c}, {"row": CORES * x + 1 - c}
    up, down = {"col": after}, {"col": before}

    barrier = pltpu.get_barrier_semaphore()
    for peer in (near, far, core, up, down):
        pl.semaphore_signal(barrier, inc=1, device_id=peer, device_id_type=MESH)
    pl.semaphore_wait(barrier, 5)

    started = []

    def send(src, dst, s_sem, r_sem, peer):
        copy = pltpu.make_async_remote_copy(src_ref=src, dst_ref=dst, send_sem=s_sem, recv_sem=r_sem, device_id=peer, device_id_type=MESH)
        copy.start()
        started.append(copy)
        return copy

    def w_slot(k, chip):
        return wo.at[k, pl.ds(pl.multiple_of((CORES * chip + c) * chunk, chunk), chunk), :]

    def w_mine(k):
        return w_ref.at[pl.ds(k * chunk, chunk), :]

    def share(k, origin, src=None):
        slot = w_slot(k, (x, xn, xf, xnf)[origin])
        return send(slot if src is None else src, slot, d_send.at[k, origin], d_recv.at[k, origin], core)

    def remote(src, dst, s_sem, r_sem, peer):
        return pltpu.make_async_remote_copy(src_ref=src, dst_ref=dst, send_sem=s_sem, recv_sem=r_sem, device_id=peer, device_id_type=MESH)

    def to_near(k):
        return remote(w_mine(k), w_slot(k, x), n_send.at[k, 0], n_recv.at[k, 0], near)

    def to_far(k):
        return remote(w_mine(k), w_slot(k, x), f_send.at[k, 0], f_recv.at[k, 0], far)

    def corner(k):
        return remote(got_ref.at[1 + k], w_slot(k, xf), n_send.at[k, 1], n_recv.at[k, 1], near)

    def begin(copy, k):
        copy(k).start()

    begin(to_near, 2)
    begin(to_far, 2)
    places = [(w_mine(k), w_slot(k, x)) for k in range(CHUNKS)]
    places += [(got_ref.at[0], w_slot(0, xn)), (got_ref.at[1], w_slot(0, xf)), (got_ref.at[2], w_slot(1, xf))]
    placed = [pltpu.make_async_copy(src, dst, l_sem.at[i]) for i, (src, dst) in enumerate(places)]
    for copy in placed:
        copy.start()
    shared = [share(k, 0, w_mine(k)) for k in range(CHUNKS)]
    shared += [share(0, 1, got_ref.at[0]), share(0, 2, got_ref.at[1]), share(1, 2, got_ref.at[2])]

    for i in range(2 * rows // 128):
        at = r if i < rows // 128 else CORES * xf + c
        line = segs_ref[at, pl.ds(i % (rows // 128), 1), :].astype(jnp.float32)
        segq[pl.ds(i * 128, 128), :] = jnp.broadcast_to(line, (128, 128)).T

    def key_row(j):
        odd, fam, plane = j % 2, (j // 2) % 2, j // 4
        base = x + fam * (xn - x)
        chip = base + odd * (n_x - 1 - 2 * base)
        return CORES * chip + c + plane * (1 - 2 * c)

    blocks = keys // rows
    lanes = rows // 128
    bufs = (buf_a, buf_b, buf_c)
    n_buf = len(bufs)

    def scores(b, u, j):
        tile, h = (u // heads + tiles // 2) % tiles, u % heads
        q = q_ref[pl.ds(pl.multiple_of(tile * Q_TILE, Q_TILE), Q_TILE), pl.ds(pl.multiple_of(h * HEAD_DIM, HEAD_DIM), HEAD_DIM)]
        k = kv_ref[pl.ds(pl.multiple_of(j * rows, rows), rows), pl.ds(0, HEAD_DIM)]
        s = lax.dot_general(q, k, (((1,), (1,)), ((), ())), preferred_element_type=jnp.float32)
        own = segq[pl.ds(pl.multiple_of(tile * Q_TILE, Q_TILE), Q_TILE), :]
        seg = segs_ref[key_row(j)].astype(jnp.float32)
        top = mbuf[b]
        for i in range(lanes):
            part = jnp.where(own == seg[i:i + 1, :], s[:, i * 128:(i + 1) * 128], lowest)
            bufs[b][j * lanes + i] = part
            top = jnp.maximum(top, part)
        mbuf[b] = top

    def powers(b, j):
        top = mbuf[b]
        total = lbuf[b]
        for i in range(lanes):
            e = jnp.exp2((bufs[b][j * lanes + i] - top) * coef)
            bufs[b][j * lanes + i] = e
            total = total + e
        lbuf[b] = total

    def context(b, j):
        inv = lbuf[b]
        p = jnp.concatenate([(bufs[b][j * lanes + i] * inv).astype(jnp.bfloat16) for i in range(lanes)], axis=1)
        v = kv_ref[pl.ds(pl.multiple_of(j * rows, rows), rows), pl.ds(HEAD_DIM, HEAD_DIM)]
        abuf[...] += jnp.dot(p, v, preferred_element_type=jnp.float32)

    def open_unit(s, a, b, e):
        if a:
            mbuf[s] = jnp.full(mbuf.shape[1:], lowest, jnp.float32)
        if b:
            lbuf[(s - 1) % n_buf] = jnp.zeros(lbuf.shape[1:], jnp.float32)
        if e:
            abuf[...] = jnp.zeros(abuf.shape, jnp.float32)

    def close_unit(s, u, a, b, e):
        if a:
            mbuf[s] = jnp.broadcast_to(jnp.max(mbuf[s], axis=1, keepdims=YES), mbuf.shape[1:])
        if b:
            lbuf[(s - 1) % n_buf] = 1.0 / jnp.broadcast_to(jnp.sum(lbuf[(s - 1) % n_buf], axis=1, keepdims=YES), lbuf.shape[1:])
        if e:
            tile, h = (u - 2) // heads, (u - 2) % heads
            out = abuf[...].astype(jnp.bfloat16)
            per = heads // CHUNKS
            lo = pl.multiple_of((h % per) * HEAD_DIM, HEAD_DIM)
            mine = pl.multiple_of((CORES * y + half) * chunk, chunk)

            at = pl.ds(pl.multiple_of(tile % (tiles // 2) * Q_TILE, Q_TILE), Q_TILE)

            @pl.when(tile >= tiles // 2)
            def _():
                panel[h // per, at, pl.ds(pl.multiple_of(mine + lo, HEAD_DIM), HEAD_DIM)] = out

            @pl.when(tile < tiles // 2)
            def _():
                obuf[h // per, at, pl.ds(lo, HEAD_DIM)] = out

    def unit(s, u, a, b, e):
        open_unit(s, a, b, e)

        @pl.loop(0, blocks // UNROLL)
        def _(jj):
            for i in range(UNROLL):
                j = jj * UNROLL + i
                if a:
                    scores(s, u, j)
                if b:
                    powers((s - 1) % n_buf, j)
                if e:
                    context((s - 2) % n_buf, j)

        close_unit(s, u, a, b, e)

    group = CHUNKS // 2

    def o_slot(yy, f, g, lo, n):
        hh = half + f * (1 - 2 * half)
        return panel.at[pl.ds(g * group, group), pl.ds(lo, n), pl.ds(pl.multiple_of((CORES * yy + hh) * chunk, chunk), chunk)]

    def send_o(a, g):
        return pltpu.make_async_remote_copy(
            src_ref=obuf.at[pl.ds(g * group, group), pl.ds(a * Q_TILE, Q_TILE), :], dst_ref=o_slot(y, 0, g, a * Q_TILE, Q_TILE),
            send_sem=t_send.at[a, g], recv_sem=t_recv.at[a, g], device_id=far, device_id_type=MESH)

    def y_copy(f, a, g, way):
        piece = o_slot(y, f, g, a * Q_TILE, Q_TILE)
        return pltpu.make_async_remote_copy(src_ref=piece, dst_ref=piece, send_sem=y_send.at[f, a, g, way], recv_sem=y_recv.at[f, a, g, way], device_id=(up, down)[way], device_id_type=MESH)

    def y_pass(f, a, g, way):
        piece = o_slot((before, after)[way], f, g, a * Q_TILE + way * eighth, eighth)
        return pltpu.make_async_remote_copy(src_ref=piece, dst_ref=piece, send_sem=y_send.at[f, a, g, 2 + way], recv_sem=y_recv.at[f, a, g, 2 + way], device_id=(up, down)[way], device_id_type=MESH)

    def w_copy(kind, k):
        if kind == 0:
            return remote(w_slot(k, xn), w_slot(k, xn), f_send.at[k, 1], f_recv.at[k, 1], far)
        slot = w_slot(k, (x, xn, xf, xnf)[kind])
        return pltpu.make_async_remote_copy(src_ref=slot, dst_ref=slot, send_sem=d_send.at[k, kind], recv_sem=d_recv.at[k, kind], device_id=core, device_id_type=MESH)

    def near_in(k):
        to_near(k).wait_recv()
        if k >= 2:
            w_copy(0, k).start()
        w_copy(1, k).start()

    def far_in(k):
        to_far(k).wait_recv()
        w_copy(2, k).start()

    def corner_in(k):
        (corner(k) if k < 2 else w_copy(0, k)).wait_recv()
        w_copy(3, k).start()

    def y_start(f, a, g):
        for way in BOTH:
            y_copy(f, a, g, way).start()

    def y_relay(f, a, g):
        for way in BOTH:
            y_copy(f, a, g, way).wait_recv()
            y_pass(f, a, g, way).start()

    def o_in(a, g):
        send_o(a, g).wait_recv()
        y_start(1, a, g)

    def o_out(a, g):
        send_o(a, g).start()

    events = (
        (3, begin, to_near, 3), (4, begin, to_far, 3), (7, o_out, 0, 0), (10, begin, to_near, 1), (11, o_out, 0, 1),
        (15, o_out, 1, 0), (16, near_in, 2), (17, begin, corner, 0), (19, o_out, 1, 1), (19, o_in, 0, 0), (20, far_in, 2),
        (21, o_in, 0, 1), (23, y_relay, 1, 0, 0), (23, y_start, 0, 0, 0), (24, begin, corner, 1), (25, near_in, 3),
        (25, y_relay, 1, 0, 1), (27, y_relay, 0, 0, 0), (27, y_start, 0, 0, 1), (28, far_in, 3), (29, near_in, 1),
        (29, o_in, 1, 0), (31, y_relay, 0, 0, 1), (31, y_start, 0, 1, 0),
    )

    unit(0, 0, YES, NO, NO)
    unit(1, 1, YES, YES, NO)

    @pl.loop(0, (units - 2) // n_buf)
    def _(i):
        for s in range(n_buf):
            for at in sorted({event[0] for event in events}):
                if (at - 2) % n_buf == s:
                    @pl.when(i == (at - 2) // n_buf)
                    def _(at=at):
                        for when, step, *which in events:
                            if when == at:
                                step(*which)
            unit((s + 2) % n_buf, 2 + i * n_buf + s, YES, YES, YES)

    unit(units % n_buf, units, NO, YES, YES)
    unit((units + 1) % n_buf, units + 1, NO, NO, YES)

    def multiply(a, k, first, last):
        tile = 2 * HEAD_DIM

        @pl.loop(0, width // tile)
        def _(n):
            cols = pl.ds(pl.multiple_of(n * tile, tile), tile)
            dot = jnp.dot(panel[k, pl.ds(a * Q_TILE, Q_TILE), :], wo[k, :, cols], preferred_element_type=jnp.float32)
            per = tile // 128
            if not first:
                dot = dot + jnp.concatenate([bufs[a][n * per + i] for i in range(per)], axis=1)
            if not last:
                for i in range(per):
                    bufs[a][n * per + i] = dot[:, i * 128:(i + 1) * 128]
            else:
                out_ref[pl.ds(a * Q_TILE, Q_TILE), cols] = dot.astype(jnp.bfloat16)

    def shares_in(k, kinds):
        for kind in kinds:
            w_copy(kind, k).wait_recv()

    def rows_in(a, g):
        for f in BOTH:
            for way in BOTH:
                y_pass(f, a, g, way).wait_recv()

    passed = (1, 2, 3)
    o_in(1, 1)
    y_start(0, 1, 1)
    y_relay(1, 1, 0)
    y_relay(0, 1, 0)
    corner_in(2)
    corner_in(0)
    for copy in placed:
        copy.wait()
    for copy in shared:
        copy.wait_recv()
    rows_in(0, 0)
    rows_in(0, 1)
    shares_in(2, passed)
    multiply(0, 2, YES, NO)
    y_relay(1, 1, 1)
    y_relay(0, 1, 1)
    shares_in(0, passed[2:])
    multiply(0, 0, NO, NO)
    rows_in(1, 0)
    multiply(1, 0, YES, NO)
    rows_in(1, 1)
    multiply(1, 2, NO, NO)
    corner_in(3)
    shares_in(3, passed)
    multiply(0, 3, NO, NO)
    corner_in(1)
    multiply(1, 3, NO, NO)
    shares_in(1, passed[::2])
    for a in BOTH:
        multiply(a, 1, NO, YES)
    for copy in started:
        copy.wait_send()
    to_near(1).wait_send()
    for k in BOTH:
        corner(k).wait_send()
    for k in (2, 3):
        to_near(k).wait_send()
        to_far(k).wait_send()
        w_copy(0, k).wait_send()
        for kind in (1, 2, 3):
            w_copy(kind, k).wait_send()
    for kind, k in ((3, 0), (1, 1), (3, 1)):
        w_copy(kind, k).wait_send()
    for a in BOTH:
        for g in BOTH:
            send_o(a, g).wait_send()
            for f in BOTH:
                for way in BOTH:
                    y_copy(f, a, g, way).wait_send()
                    y_pass(f, a, g, way).wait_send()


def attend_project(q, kv, segs, got, w_out, n_x, n_y):
    rows, ctx = q.shape[0] // 2, q.shape[1]
    keys = kv.shape[0]
    depth, width = w_out.shape
    n_row = CORES * n_x
    chunk = depth // CHUNKS
    dma = pltpu.SemaphoreType.DMA
    anywhere, vmem = pl.BlockSpec(memory_space=pl.ANY), pl.BlockSpec(memory_space=pltpu.VMEM)
    return pl.pallas_call(
        functools.partial(attend_kernel, n_x, n_y),
        out_shape=jax.ShapeDtypeStruct((rows, width), jnp.bfloat16),
        in_specs=[vmem, vmem, vmem, anywhere, anywhere],
        out_specs=vmem,
        scratch_shapes=[
            pltpu.VMEM((CHUNKS, n_row * chunk, width), jnp.bfloat16),
            pltpu.VMEM((CHUNKS, rows, n_row * chunk), jnp.bfloat16),
            pltpu.VMEM((CHUNKS, rows, chunk), jnp.bfloat16),
            pltpu.VMEM((keys // 128, Q_TILE, 128), jnp.float32),
            pltpu.VMEM((keys // 128, Q_TILE, 128), jnp.float32),
            pltpu.VMEM((keys // 128, Q_TILE, 128), jnp.float32),
            pltpu.VMEM((2 * rows, 128), jnp.float32),
            pltpu.VMEM((3, Q_TILE, 128), jnp.float32),
            pltpu.VMEM((3, Q_TILE, 128), jnp.float32),
            pltpu.VMEM((Q_TILE, HEAD_DIM), jnp.float32),
            *[dma(shape) for shape in ((CHUNKS, 2), (CHUNKS, 2), (CHUNKS, 4), (2, 2), (2, 2, 2, 4)) for _ in BOTH],
            dma((CHUNKS + 3,)),
        ],
        compiler_params=pltpu.CompilerParams(collective_id=1, has_side_effects=YES, vmem_limit_bytes=63 * 1024 * 1024),
        cost_estimate=pl.CostEstimate(flops=8 * rows * ctx * keys, bytes_accessed=4 * depth * width, transcendentals=0),
        name="attend_project",
    )(q, kv, segs, got, w_out)


def solution(mesh):
    n_x, n_y = mesh.shape["row"] // CORES, mesh.shape["col"]

    def local_block(tokens, w_qkv, w_out, doc_ids):
        q, kv, segs, got = project_qkv(tokens, w_qkv, w_out, doc_ids, n_x, n_y)
        return attend_project(q, kv, segs, got, w_out, n_x, n_y)

    row_spec = P(("data", "row"), "col")
    weight_spec = P("row", "col")
    return jax.shard_map(local_block, mesh=mesh, in_specs=(row_spec, weight_spec, weight_spec, P(("data", "row"))), out_specs=row_spec, check_vma=NO)
```

```python
import functools

import jax
import jax.numpy as jnp
from jax import lax
from jax.experimental import pallas as pl
from jax.experimental.pallas import tpu as pltpu
from jax.sharding import PartitionSpec as P

HEAD_DIM = 128
CORES = 2
Q_TILE = 256
CHUNKS = 4
UNROLL = 4
LOG2E = 1.4426950408889634
BOTH = (0, 1)
YES, NO = True, False


MESH = pl.DeviceIdType.MESH


def near_x(x):
    return x + 1 - 2 * (x % 2)


def qkv_kernel(n_x, n_y, tok_ref, w_ref, wo_ref, seg_ref, q_ref, kv_ref, segs_ref, got_ref, xg, wg, acc, w_send, w_recv, d_send, d_recv, t_send, t_recv, y_send, y_recv, k_send, k_recv, s_send, s_recv, o_send, o_recv, l_sem):
    r, y = lax.axis_index("row"), lax.axis_index("col")
    x, c = r // CORES, r % CORES
    xn, xf = near_x(x), n_x - 1 - x
    xnf = n_x - 1 - xn
    half = x // (n_x // 2)
    before, after, across = (y + n_y - 1) % n_y, (y + 1) % n_y, (y + 2) % n_y
    rows, width = tok_ref.shape
    depth = w_ref.shape[0]
    part = w_ref.shape[1] // 2
    ctx = part - 2 * HEAD_DIM
    mid, cut, quarter = rows // 2, depth // 2, rows // 4
    near, far, core = {"row": CORES * xn + c}, {"row": CORES * xf + c}, {"row": CORES * x + 1 - c}
    up, down = {"col": after}, {"col": before}

    barrier = pltpu.get_barrier_semaphore()
    n_row = CORES * n_x
    row_peers = [{"row": (r + d) % n_row} for d in range(1, n_row)]
    for peer in row_peers + [up, down]:
        pl.semaphore_signal(barrier, inc=1, device_id=peer, device_id_type=MESH)
    pl.semaphore_wait(barrier, n_row + 1)

    started = []

    def send(src, dst, s_sem, r_sem, peer):
        copy = pltpu.make_async_remote_copy(src_ref=src, dst_ref=dst, send_sem=s_sem, recv_sem=r_sem, device_id=peer, device_id_type=MESH)
        copy.start()
        started.append(copy)
        return copy

    mine = pl.ds(pl.multiple_of(half * part, 128), part)
    theirs = pl.ds(pl.multiple_of((1 - half) * part, 128), part)

    def w_slot(chip, plane, i):
        return wg.at[chip, pl.ds(pl.multiple_of(plane * depth + i * cut, cut), cut), :]

    def send_w(kind, i):
        src_rows = pl.ds(i * cut, cut)
        if kind == 0:
            return send(w_ref.at[src_rows, mine], w_slot(x, c, i), w_send.at[0, i], w_recv.at[0, i], near)
        if kind == 1:
            return send(w_ref.at[src_rows, theirs], w_slot(x, c, i), w_send.at[1, i], w_recv.at[1, i], far)
        return send(w_slot(xf, c, i), w_slot(xf, c, i), w_send.at[2, i], w_recv.at[2, i], near)

    def share(chip, i, at):
        src = w_ref.at[pl.ds(i * cut, cut), mine] if at == 0 else w_slot(chip, c, i)
        return send(src, w_slot(chip, c, i), d_send.at[at, i], d_recv.at[at, i], core)

    def x_slot(b, at, lo, n):
        return xg.at[b, at, pl.ds(lo, n), :]

    def send_t(a):
        return send(tok_ref.at[pl.ds(a * mid, mid), :], x_slot(1, y, a * mid, mid), t_send.at[a], t_recv.at[a], far)

    def send_y(b, a, way):
        src = tok_ref.at[pl.ds(a * mid, mid), :] if b == 0 else x_slot(1, y, a * mid, mid)
        return send(src, x_slot(b, y, a * mid, mid), y_send.at[b, a, way], y_recv.at[b, a, way], (up, down)[way])

    def pass_y(b, a, way):
        at = (before, after)[way]
        piece = x_slot(b, at, a * mid + way * quarter, quarter)
        return send(piece, piece, y_send.at[b, a, 2 + way], y_recv.at[b, a, 2 + way], (up, down)[way])

    segs = [send(seg_ref, segs_ref.at[r], s_send.at[d], s_recv.at[d], peer) for d, peer in enumerate(row_peers)]
    w_far = [send_w(1, 0)]
    y_own = [[send_y(0, a, way) for way in BOTH] for a in BOTH]
    w_near = [send_w(0, 0)]
    tok = [send_t(0)]
    w_near.append(send_w(0, 1))
    w_far.append(send_w(1, 1))
    tok.append(send_t(1))
    chunk = depth // CHUNKS
    locals_ = [
        pltpu.make_async_copy(seg_ref, segs_ref.at[r], l_sem.at[2]),
        pltpu.make_async_copy(tok_ref, xg.at[0, y], l_sem.at[0]),
        pltpu.make_async_copy(w_ref.at[:, mine], wg.at[x, pl.ds(pl.multiple_of(c * depth, depth), depth), :], l_sem.at[1]),
    ]
    for copy in locals_:
        copy.start()
    d_own = [share(x, i, 0) for i in BOTH]

    def multiply(b, lo, n, chip, first, last):
        tile = 2 * HEAD_DIM

        @pl.loop(0, part // tile)
        def _(j):
            cols = pl.ds(pl.multiple_of(j * tile, tile), tile)
            dot = jnp.dot(xg[b, chip, pl.ds(lo, n), :], wg[chip, :, cols], preferred_element_type=jnp.float32)
            if not first:
                dot = dot + acc[pl.ds(lo, n), cols]
            if not last:
                acc[pl.ds(lo, n), cols] = dot
            else:
                out = dot.astype(jnp.bfloat16)

                @pl.when(j < ctx // tile)
                def _():
                    q_ref[pl.ds(b * rows + lo, n), cols] = out

                @pl.when(j == ctx // tile)
                def _():
                    kv_ref[pl.ds(b * rows + lo, n), :] = out

    def kv_slot(s):
        return kv_ref.at[pl.ds(s * rows, rows), :]

    def kv_near(b):
        return send(kv_slot(b), kv_slot(2 + b), k_send.at[b], k_recv.at[b], near)

    def kv_core(s):
        return send(kv_slot(s), kv_slot(4 + s), k_send.at[2 + s], k_recv.at[2 + s], core)

    def relay(b, a):
        got = []
        for way in BOTH:
            (y_own if b == 0 else y_par)[a][way].wait_recv()
            got.append(pass_y(b, a, way))
        return got

    y_far = [relay(0, 0)]
    w_far[0].wait_recv()
    w_nf = [send_w(2, 0)]
    d_far = [share(xf, 0, 2)]
    w_near[0].wait_recv()
    d_near = [share(xn, 0, 1)]
    y_far.append(relay(0, 1))
    tok[0].wait_recv()
    y_par = [[send_y(1, 0, way) for way in BOTH]]
    wo_got = [send(wo_ref.at[pl.ds(i * chunk, chunk), :], got_ref.at[1 + i], o_send.at[1 + i], o_recv.at[1 + i], far) for i in BOTH]
    w_near[1].wait_recv()
    d_near.append(share(xn, 1, 1))
    for pair in y_far:
        for copy in pair:
            copy.wait_recv()
    for copy in locals_:
        copy.wait()
    for copy in d_own:
        copy.wait_recv()
    multiply(0, 0, rows, x, YES, NO)
    for copy in d_near:
        copy.wait_recv()
    w_far[1].wait_recv()
    w_nf.append(send_w(2, 1))
    wo_got.append(send(wo_ref.at[pl.ds(0, chunk), :], got_ref.at[0], o_send.at[0], o_recv.at[0], near))
    d_far.append(share(xf, 1, 2))
    multiply(0, 0, rows, xn, NO, NO)
    w_nf[0].wait_recv()
    d_nf = [share(xnf, 0, 3)]
    y_pfar = [relay(1, 0)]
    tok[1].wait_recv()
    y_par.append([send_y(1, 1, way) for way in BOTH])
    for copy in d_far:
        copy.wait_recv()
    multiply(0, 0, rows, xf, NO, NO)
    w_nf[1].wait_recv()
    d_nf.append(share(xnf, 1, 3))
    for copy in d_nf:
        copy.wait_recv()
    multiply(0, 0, rows, xnf, NO, YES)
    for copy in y_pfar[0]:
        copy.wait_recv()
    multiply(1, 0, mid, y, YES, NO)
    k_near, k_core = [kv_near(0)], [kv_core(0)]
    multiply(1, 0, mid, before, NO, NO)
    y_pfar.append(relay(1, 1))
    multiply(1, 0, mid, after, NO, NO)
    multiply(1, 0, mid, across, NO, YES)
    multiply(1, mid, mid, y, YES, NO)
    multiply(1, mid, mid, before, NO, NO)
    multiply(1, mid, mid, after, NO, NO)
    k_near[0].wait_recv()
    k_core.append(kv_core(2))
    for copy in y_pfar[1]:
        copy.wait_recv()
    multiply(1, mid, mid, across, NO, YES)
    k_near.append(kv_near(1))
    k_core.append(kv_core(1))
    k_near[1].wait_recv()
    k_core.append(kv_core(3))
    for copy in k_core + wo_got + segs:
        copy.wait_recv()
    for copy in started:
        copy.wait_send()


def project_qkv(tokens, w_qkv, w_out, doc_ids, n_x, n_y):
    rows, width = tokens.shape
    depth, cols = w_qkv.shape
    part = cols // 2
    ctx = part - 2 * HEAD_DIM
    n_row = CORES * n_x
    dma = pltpu.SemaphoreType.DMA
    anywhere, vmem = pl.BlockSpec(memory_space=pl.ANY), pl.BlockSpec(memory_space=pltpu.VMEM)
    segs = doc_ids.reshape(rows // 128, 128)
    return pl.pallas_call(
        functools.partial(qkv_kernel, n_x, n_y),
        out_shape=(
            jax.ShapeDtypeStruct((2 * rows, ctx), jnp.bfloat16),
            jax.ShapeDtypeStruct((n_row * rows, 2 * HEAD_DIM), jnp.bfloat16),
            jax.ShapeDtypeStruct((n_row,) + segs.shape, jnp.int32),
            jax.ShapeDtypeStruct((3, depth // CHUNKS, w_out.shape[1]), jnp.bfloat16),
        ),
        in_specs=[anywhere] * 4,
        out_specs=(vmem, vmem, vmem, anywhere),
        scratch_shapes=[
            pltpu.VMEM((2, n_y, rows, width), jnp.bfloat16),
            pltpu.VMEM((n_x, CORES * depth, part), jnp.bfloat16),
            pltpu.VMEM((rows, part), jnp.float32),
            *[dma(shape) for shape in ((3, 2), (4, 2), (2,), (2, 2, 4), (6,), (n_row - 1,), (3,)) for _ in BOTH],
            dma((3,)),
        ],
        compiler_params=pltpu.CompilerParams(collective_id=0, has_side_effects=YES, vmem_limit_bytes=60 * 1024 * 1024),
        cost_estimate=pl.CostEstimate(flops=4 * rows * n_y * width * part, bytes_accessed=2 * depth * cols, transcendentals=0),
        name="project_qkv",
    )(tokens, w_qkv, w_out, segs)


def attend_kernel(n_x, n_y, q_ref, kv_ref, segs_ref, got_ref, w_ref, out_ref, wo, panel, obuf, buf_a, buf_b, buf_c, segq, mbuf, lbuf, abuf, n_send, n_recv, f_send, f_recv, d_send, d_recv, t_send, t_recv, y_send, y_recv, l_sem):
    r, y = lax.axis_index("row"), lax.axis_index("col")
    x, c = r // CORES, r % CORES
    xn, xf = near_x(x), n_x - 1 - x
    xnf = n_x - 1 - xn
    half = x // (n_x // 2)
    before, after, across = (y + n_y - 1) % n_y, (y + 1) % n_y, (y + 2) % n_y
    rows = out_ref.shape[0]
    keys = kv_ref.shape[0]
    chunk = w_ref.shape[0] // CHUNKS
    width = w_ref.shape[1]
    heads = q_ref.shape[1] // HEAD_DIM
    tiles = 2 * rows // Q_TILE
    units = tiles * heads
    eighth = Q_TILE // 2
    coef = HEAD_DIM ** -0.5 * LOG2E
    lowest = jnp.finfo(jnp.float32).min
    near, far, core = {"row": CORES * xn + c}, {"row": CORES * xf + c}, {"row": CORES * x + 1 - c}
    up, down = {"col": after}, {"col": before}

    barrier = pltpu.get_barrier_semaphore()
    for peer in (near, far, core, up, down):
        pl.semaphore_signal(barrier, inc=1, device_id=peer, device_id_type=MESH)
    pl.semaphore_wait(barrier, 5)

    started = []

    def send(src, dst, s_sem, r_sem, peer):
        copy = pltpu.make_async_remote_copy(src_ref=src, dst_ref=dst, send_sem=s_sem, recv_sem=r_sem, device_id=peer, device_id_type=MESH)
        copy.start()
        started.append(copy)
        return copy

    def w_slot(k, chip):
        return wo.at[k, pl.ds(pl.multiple_of((CORES * chip + c) * chunk, chunk), chunk), :]

    def w_mine(k):
        return w_ref.at[pl.ds(k * chunk, chunk), :]

    def share(k, origin, src=None):
        slot = w_slot(k, (x, xn, xf, xnf)[origin])
        return send(slot if src is None else src, slot, d_send.at[k, origin], d_recv.at[k, origin], core)

    def remote(src, dst, s_sem, r_sem, peer):
        return pltpu.make_async_remote_copy(src_ref=src, dst_ref=dst, send_sem=s_sem, recv_sem=r_sem, device_id=peer, device_id_type=MESH)

    def to_near(k):
        return remote(w_mine(k), w_slot(k, x), n_send.at[k, 0], n_recv.at[k, 0], near)

    def to_far(k):
        return remote(w_mine(k), w_slot(k, x), f_send.at[k, 0], f_recv.at[k, 0], far)

    def corner(k):
        return remote(got_ref.at[1 + k], w_slot(k, xf), n_send.at[k, 1], n_recv.at[k, 1], near)

    def begin(copy, k):
        copy(k).start()

    begin(to_near, 2)
    begin(to_far, 2)
    places = [(w_mine(k), w_slot(k, x)) for k in range(CHUNKS)]
    places += [(got_ref.at[0], w_slot(0, xn)), (got_ref.at[1], w_slot(0, xf)), (got_ref.at[2], w_slot(1, xf))]
    placed = [pltpu.make_async_copy(src, dst, l_sem.at[i]) for i, (src, dst) in enumerate(places)]
    for copy in placed:
        copy.start()
    shared = [share(k, 0, w_mine(k)) for k in range(CHUNKS)]
    shared += [share(0, 1, got_ref.at[0]), share(0, 2, got_ref.at[1]), share(1, 2, got_ref.at[2])]

    for i in range(2 * rows // 128):
        at = r if i < rows // 128 else CORES * xf + c
        line = segs_ref[at, pl.ds(i % (rows // 128), 1), :].astype(jnp.float32)
        segq[pl.ds(i * 128, 128), :] = jnp.broadcast_to(line, (128, 128)).T

    def key_row(j):
        odd, fam, plane = j % 2, (j // 2) % 2, j // 4
        base = x + fam * (xn - x)
        chip = base + odd * (n_x - 1 - 2 * base)
        return CORES * chip + c + plane * (1 - 2 * c)

    blocks = keys // rows
    lanes = rows // 128
    bufs = (buf_a, buf_b, buf_c)
    n_buf = len(bufs)

    def scores(b, u, j):
        tile, h = (u // heads + tiles // 2) % tiles, u % heads
        q = q_ref[pl.ds(pl.multiple_of(tile * Q_TILE, Q_TILE), Q_TILE), pl.ds(pl.multiple_of(h * HEAD_DIM, HEAD_DIM), HEAD_DIM)]
        k = kv_ref[pl.ds(pl.multiple_of(j * rows, rows), rows), pl.ds(0, HEAD_DIM)]
        s = lax.dot_general(q, k, (((1,), (1,)), ((), ())), preferred_element_type=jnp.float32)
        own = segq[pl.ds(pl.multiple_of(tile * Q_TILE, Q_TILE), Q_TILE), :]
        seg = segs_ref[key_row(j)].astype(jnp.float32)
        top = mbuf[b]
        for i in range(lanes):
            part = jnp.where(own == seg[i:i + 1, :], s[:, i * 128:(i + 1) * 128], lowest)
            bufs[b][j * lanes + i] = part
            top = jnp.maximum(top, part)
        mbuf[b] = top

    def powers(b, j):
        top = mbuf[b]
        total = lbuf[b]
        for i in range(lanes):
            e = jnp.exp2((bufs[b][j * lanes + i] - top) * coef)
            bufs[b][j * lanes + i] = e
            total = total + e
        lbuf[b] = total

    def context(b, j):
        inv = lbuf[b]
        p = jnp.concatenate([(bufs[b][j * lanes + i] * inv).astype(jnp.bfloat16) for i in range(lanes)], axis=1)
        v = kv_ref[pl.ds(pl.multiple_of(j * rows, rows), rows), pl.ds(HEAD_DIM, HEAD_DIM)]
        abuf[...] += jnp.dot(p, v, preferred_element_type=jnp.float32)

    def open_unit(s, a, b, e):
        if a:
            mbuf[s] = jnp.full(mbuf.shape[1:], lowest, jnp.float32)
        if b:
            lbuf[(s - 1) % n_buf] = jnp.zeros(lbuf.shape[1:], jnp.float32)
        if e:
            abuf[...] = jnp.zeros(abuf.shape, jnp.float32)

    def close_unit(s, u, a, b, e):
        if a:
            mbuf[s] = jnp.broadcast_to(jnp.max(mbuf[s], axis=1, keepdims=YES), mbuf.shape[1:])
        if b:
            lbuf[(s - 1) % n_buf] = 1.0 / jnp.broadcast_to(jnp.sum(lbuf[(s - 1) % n_buf], axis=1, keepdims=YES), lbuf.shape[1:])
        if e:
            tile, h = (u - 2) // heads, (u - 2) % heads
            out = abuf[...].astype(jnp.bfloat16)
            per = heads // CHUNKS
            lo = pl.multiple_of((h % per) * HEAD_DIM, HEAD_DIM)
            mine = pl.multiple_of((CORES * y + half) * chunk, chunk)

            at = pl.ds(pl.multiple_of(tile % (tiles // 2) * Q_TILE, Q_TILE), Q_TILE)

            @pl.when(tile >= tiles // 2)
            def _():
                panel[h // per, at, pl.ds(pl.multiple_of(mine + lo, HEAD_DIM), HEAD_DIM)] = out

            @pl.when(tile < tiles // 2)
            def _():
                obuf[h // per, at, pl.ds(lo, HEAD_DIM)] = out

    def unit(s, u, a, b, e):
        open_unit(s, a, b, e)

        @pl.loop(0, blocks // UNROLL)
        def _(jj):
            for i in range(UNROLL):
                j = jj * UNROLL + i
                if a:
                    scores(s, u, j)
                if b:
                    powers((s - 1) % n_buf, j)
                if e:
                    context((s - 2) % n_buf, j)

        close_unit(s, u, a, b, e)

    group = CHUNKS // 2

    def o_slot(yy, f, g, lo, n):
        hh = half + f * (1 - 2 * half)
        return panel.at[pl.ds(g * group, group), pl.ds(lo, n), pl.ds(pl.multiple_of((CORES * yy + hh) * chunk, chunk), chunk)]

    def send_o(a, g):
        return pltpu.make_async_remote_copy(
            src_ref=obuf.at[pl.ds(g * group, group), pl.ds(a * Q_TILE, Q_TILE), :], dst_ref=o_slot(y, 0, g, a * Q_TILE, Q_TILE),
            send_sem=t_send.at[a, g], recv_sem=t_recv.at[a, g], device_id=far, device_id_type=MESH)

    def y_copy(f, a, g, way):
        piece = o_slot(y, f, g, a * Q_TILE, Q_TILE)
        return pltpu.make_async_remote_copy(src_ref=piece, dst_ref=piece, send_sem=y_send.at[f, a, g, way], recv_sem=y_recv.at[f, a, g, way], device_id=(up, down)[way], device_id_type=MESH)

    def y_pass(f, a, g, way):
        piece = o_slot((before, after)[way], f, g, a * Q_TILE + way * eighth, eighth)
        return pltpu.make_async_remote_copy(src_ref=piece, dst_ref=piece, send_sem=y_send.at[f, a, g, 2 + way], recv_sem=y_recv.at[f, a, g, 2 + way], device_id=(up, down)[way], device_id_type=MESH)

    def w_copy(kind, k):
        if kind == 0:
            return remote(w_slot(k, xn), w_slot(k, xn), f_send.at[k, 1], f_recv.at[k, 1], far)
        slot = w_slot(k, (x, xn, xf, xnf)[kind])
        return pltpu.make_async_remote_copy(src_ref=slot, dst_ref=slot, send_sem=d_send.at[k, kind], recv_sem=d_recv.at[k, kind], device_id=core, device_id_type=MESH)

    def near_in(k):
        to_near(k).wait_recv()
        if k >= 2:
            w_copy(0, k).start()
        w_copy(1, k).start()

    def far_in(k):
        to_far(k).wait_recv()
        w_copy(2, k).start()

    def corner_in(k):
        (corner(k) if k < 2 else w_copy(0, k)).wait_recv()
        w_copy(3, k).start()

    def y_start(f, a, g):
        for way in BOTH:
            y_copy(f, a, g, way).start()

    def y_relay(f, a, g):
        for way in BOTH:
            y_copy(f, a, g, way).wait_recv()
            y_pass(f, a, g, way).start()

    def o_in(a, g):
        send_o(a, g).wait_recv()
        y_start(1, a, g)

    def o_out(a, g):
        send_o(a, g).start()

    events = (
        (3, begin, to_near, 3), (4, begin, to_far, 3), (7, o_out, 0, 0), (10, begin, to_near, 1), (11, o_out, 0, 1),
        (15, o_out, 1, 0), (16, near_in, 2), (17, begin, corner, 0), (19, o_out, 1, 1), (19, o_in, 0, 0), (20, far_in, 2),
        (21, o_in, 0, 1), (23, y_relay, 1, 0, 0), (23, y_start, 0, 0, 0), (24, begin, corner, 1), (25, near_in, 3),
        (25, y_relay, 1, 0, 1), (27, y_relay, 0, 0, 0), (27, y_start, 0, 0, 1), (28, far_in, 3), (29, near_in, 1),
        (29, o_in, 1, 0), (31, y_relay, 0, 0, 1), (31, y_start, 0, 1, 0),
    )

    unit(0, 0, YES, NO, NO)
    unit(1, 1, YES, YES, NO)

    @pl.loop(0, (units - 2) // n_buf)
    def _(i):
        for s in range(n_buf):
            for at in sorted({event[0] for event in events}):
                if (at - 2) % n_buf == s:
                    @pl.when(i == (at - 2) // n_buf)
                    def _(at=at):
                        for when, step, *which in events:
                            if when == at:
                                step(*which)
            unit((s + 2) % n_buf, 2 + i * n_buf + s, YES, YES, YES)

    unit(units % n_buf, units, NO, YES, YES)
    unit((units + 1) % n_buf, units + 1, NO, NO, YES)

    def multiply(a, k, first, last):
        tile = 2 * HEAD_DIM

        @pl.loop(0, width // tile)
        def _(n):
            cols = pl.ds(pl.multiple_of(n * tile, tile), tile)
            dot = jnp.dot(panel[k, pl.ds(a * Q_TILE, Q_TILE), :], wo[k, :, cols], preferred_element_type=jnp.float32)
            per = tile // 128
            if not first:
                dot = dot + jnp.concatenate([bufs[a][n * per + i] for i in range(per)], axis=1)
            if not last:
                for i in range(per):
                    bufs[a][n * per + i] = dot[:, i * 128:(i + 1) * 128]
            else:
                out_ref[pl.ds(a * Q_TILE, Q_TILE), cols] = dot.astype(jnp.bfloat16)

    def shares_in(k, kinds):
        for kind in kinds:
            w_copy(kind, k).wait_recv()

    def rows_in(a, g):
        for f in BOTH:
            for way in BOTH:
                y_pass(f, a, g, way).wait_recv()

    passed = (1, 2, 3)
    o_in(1, 1)
    y_start(0, 1, 1)
    y_relay(1, 1, 0)
    y_relay(0, 1, 0)
    corner_in(2)
    corner_in(0)
    for copy in placed:
        copy.wait()
    for copy in shared:
        copy.wait_recv()
    rows_in(0, 0)
    rows_in(0, 1)
    shares_in(2, passed)
    multiply(0, 2, YES, NO)
    y_relay(1, 1, 1)
    y_relay(0, 1, 1)
    shares_in(0, passed[2:])
    multiply(0, 0, NO, NO)
    rows_in(1, 0)
    multiply(1, 0, YES, NO)
    rows_in(1, 1)
    multiply(1, 2, NO, NO)
    corner_in(3)
    shares_in(3, passed)
    multiply(0, 3, NO, NO)
    corner_in(1)
    multiply(1, 3, NO, NO)
    shares_in(1, passed[::2])
    for a in BOTH:
        multiply(a, 1, NO, YES)
    for copy in started:
        copy.wait_send()
    to_near(1).wait_send()
    for k in BOTH:
        corner(k).wait_send()
    for k in (2, 3):
        to_near(k).wait_send()
        to_far(k).wait_send()
        w_copy(0, k).wait_send()
        for kind in (1, 2, 3):
            w_copy(kind, k).wait_send()
    for kind, k in ((3, 0), (1, 1), (3, 1)):
        w_copy(kind, k).wait_send()
    for a in BOTH:
        for g in BOTH:
            send_o(a, g).wait_send()
            for f in BOTH:
                for way in BOTH:
                    y_copy(f, a, g, way).wait_send()
                    y_pass(f, a, g, way).wait_send()


def attend_project(q, kv, segs, got, w_out, n_x, n_y):
    rows, ctx = q.shape[0] // 2, q.shape[1]
    keys = kv.shape[0]
    depth, width = w_out.shape
    n_row = CORES * n_x
    chunk = depth // CHUNKS
    dma = pltpu.SemaphoreType.DMA
    anywhere, vmem = pl.BlockSpec(memory_space=pl.ANY), pl.BlockSpec(memory_space=pltpu.VMEM)
    return pl.pallas_call(
        functools.partial(attend_kernel, n_x, n_y),
        out_shape=jax.ShapeDtypeStruct((rows, width), jnp.bfloat16),
        in_specs=[vmem, vmem, vmem, anywhere, anywhere],
        out_specs=vmem,
        scratch_shapes=[
            pltpu.VMEM((CHUNKS, n_row * chunk, width), jnp.bfloat16),
            pltpu.VMEM((CHUNKS, rows, n_row * chunk), jnp.bfloat16),
            pltpu.VMEM((CHUNKS, rows, chunk), jnp.bfloat16),
            pltpu.VMEM((keys // 128, Q_TILE, 128), jnp.float32),
            pltpu.VMEM((keys // 128, Q_TILE, 128), jnp.float32),
            pltpu.VMEM((keys // 128, Q_TILE, 128), jnp.float32),
            pltpu.VMEM((2 * rows, 128), jnp.float32),
            pltpu.VMEM((3, Q_TILE, 128), jnp.float32),
            pltpu.VMEM((3, Q_TILE, 128), jnp.float32),
            pltpu.VMEM((Q_TILE, HEAD_DIM), jnp.float32),
            *[dma(shape) for shape in ((CHUNKS, 2), (CHUNKS, 2), (CHUNKS, 4), (2, 2), (2, 2, 2, 4)) for _ in BOTH],
            dma((CHUNKS + 3,)),
        ],
        compiler_params=pltpu.CompilerParams(collective_id=1, has_side_effects=YES, vmem_limit_bytes=63 * 1024 * 1024),
        cost_estimate=pl.CostEstimate(flops=8 * rows * ctx * keys, bytes_accessed=4 * depth * width, transcendentals=0),
        name="attend_project",
    )(q, kv, segs, got, w_out)


def solution(mesh):
    n_x, n_y = mesh.shape["row"] // CORES, mesh.shape["col"]

    def local_block(tokens, w_qkv, w_out, doc_ids):
        q, kv, segs, got = project_qkv(tokens, w_qkv, w_out, doc_ids, n_x, n_y)
        return attend_project(q, kv, segs, got, w_out, n_x, n_y)

    row_spec = P(("data", "row"), "col")
    weight_spec = P("row", "col")
    return jax.shard_map(local_block, mesh=mesh, in_specs=(row_spec, weight_spec, weight_spec, P(("data", "row"))), out_specs=row_spec, check_vma=NO)
```
